256 devices in a mesh: grp: 2 (over y), seq: 128 (over z, x, core).
Axes of the slice: x: 4, y: 2, z: 16, core: 2. Of those that a mesh axis runs over, the one named last changes fastest.
The devices are a block of a 4x16x16 slice.
Arguments:
- history: bfloat16 [65536, 1024], P(('grp', 'seq')), parts along dimension 0, may hold values from -6 to 6
- candidates: bfloat16 [4096, 1024], P(('grp', 'seq')), parts along dimension 0, may hold values from -6 to 6
- lengths: int32 [8], P('grp'), parts along dimension 0, may hold values from 1 to 16384, 32768 in all
- cand_user: int32 [4096], P(('grp', 'seq')), parts along dimension 0, may hold values from 0 to 3
- w_in: bfloat16 [1, 1024, 4096], replicated, may hold values from -0.125 to 0.125
- w_out: bfloat16 [1, 1024, 1024], replicated, may hold values from -0.1875 to 0.1875
Outputs:
- history_out: bfloat16 [65536, 1024], P(('grp', 'seq')), parts along dimension 0
- cand_out: bfloat16 [4096, 1024], P(('grp', 'seq')), parts along dimension 0
The draws below stay inside these ranges and needn't reach their ends.
There are 2 independent parts, one for each index of `grp`. The reference program is written for one: setup_inputs(seed, part) draws one part's arguments, and reference() takes and returns one part's arrays. A program takes and returns all parts, laid end to end along the dimension named above; an argument that names none is the same for every part. Nothing has to cross between parts.
Inputs may be any that keep to these rules, and one draw needn't show every extreme that they name: Each user's history length is at least 1; the lengths sum to 32768, and one of them is exactly 16384.
All inputs are finite; a program needn't handle non-finite values.
Results may differ from the reference program's by a relative error of at most 0.0075.
Values may be sent and summed in bfloat16 or wider, within the bound.
A program may use at most 128 MiB of HBM per device.

```python
import math
import jax
import jax.numpy as jnp
import numpy as np
from jax import lax

D = 1024
HEADS = 8
HEAD_DIM = 128
LAYERS = 1
TOK_DEV = 256
HIST = 32768
WIN = 8
SPAN = 1792
USERS = 4
MOSTLEN = 16384
CANDS = 2048
N_SEQ = 128


def draw_w_in(key, part):
    noise_key = jax.random.fold_in(key, 11)
    head_key = jax.random.fold_in(key, 23)
    independent = jax.random.normal(noise_key, (LAYERS, D, 4 * D), jnp.float32)
    weight_share = 0.7
    common = jax.random.normal(head_key, (LAYERS, D, 2, HEADS, 1), jnp.float32)
    common = jnp.broadcast_to(common, (LAYERS, D, 2, HEADS, D // HEADS)).reshape(LAYERS, D, 2 * D)
    query_key = weight_share * common + (1.0 - weight_share * weight_share) ** 0.5 * independent[:, :, 2 * D:]
    complete = jnp.concatenate([independent[:, :, 0:2 * D], query_key], axis=2)
    return (jnp.clip(complete, -4.0, 4.0) * D ** (-0.5)).astype(jnp.bfloat16)


def with_ends(drawn, key, low, high):
    dims = drawn.shape
    spot = [jax.random.randint(jax.random.fold_in(key, axis), (), 0, dims[axis]) for axis in range(len(dims))]
    drawn = drawn.at[tuple(spot)].set(low)
    longest = dims.index(max(dims))
    spot[longest] = (spot[longest] + 1) % dims[longest]
    return drawn.at[tuple(spot)].set(high)


def block_levels(rng, extent, cuts, low, high):
    def one(axis_at, parts):
        steps = jax.random.uniform(jax.random.fold_in(jax.random.fold_in(rng, 6), axis_at), (parts,), jnp.float32, low / len(cuts), high / len(cuts))
        return jnp.repeat(jnp.exp(steps), extent[axis_at] // parts).reshape((-1,) + (1,) * (len(extent) - axis_at - 1))

    level = one(*cuts[0])
    for cut in cuts[1:]:
        level = level * one(*cut)
    return level


def profile(number_of, total, reach, skew):
    portions = [(1 << 20) // math.isqrt(standing ** skew) + 1 for standing in range(2, number_of + 1)]
    surplus, counts = total - reach - (number_of - 1), [1] * (number_of - 1)
    while surplus > 0:
        free = [i for i in range(number_of - 1) if counts[i] < reach]
        pool, left = sum([portions[i] for i in free]), surplus
        for i in free:
            addition = min(reach - counts[i], max(1, left * portions[i] // pool), surplus)
            counts[i] = counts[i] + addition
            surplus = surplus - addition
    return np.array([reach] + counts)


def ragged(rng, amount, total, most, lean):
    if amount == 2:
        one = jax.random.randint(rng, (), max(1, total - most), min(most, total - 1) + 1)
        return jnp.stack([one, total - one])
    sizes = jnp.asarray(profile(amount, total, most, lean), jnp.int32)
    couples = (amount - 1) // 2
    donor, receiver = sizes[1:1 + 2 * couples:2], sizes[2:2 + 2 * couples:2]
    slack = jnp.minimum(donor - 1, most - receiver)
    passed = jax.random.randint(jax.random.fold_in(rng, 1), (couples,), 0, 1 << 20) % (slack + 1)
    sizes = sizes.at[1:1 + 2 * couples:2].set(donor - passed).at[2:2 + 2 * couples:2].set(receiver + passed)
    return sizes[jax.random.permutation(jax.random.fold_in(rng, 2), amount)]


def noise(stream_key, dims, deviation, reach, split=(), kind=jnp.bfloat16):
    loudness = block_levels(stream_key, dims, split, -0.22, 0.18) if split else 1.0
    array = jax.random.normal(stream_key, dims, jnp.float32) * deviation * loudness
    return jnp.minimum(jnp.maximum(array, -reach), reach).astype(kind)


def setup_inputs(seed: int = 0, part: int = 0) -> dict:
    key_list = jax.random.split(jax.random.key(seed), 7)
    own_keys = jax.random.split(jax.random.fold_in(key_list[6], part), 7)
    history = noise(own_keys[0], (HIST, D), 1.0, 6.0, ((0, 128),))
    candidates = noise(own_keys[1], (CANDS, D), 1.0, 6.0, ((0, 128),))
    lengths = ragged(own_keys[2], USERS, HIST, MOSTLEN, 2).astype(jnp.int32)
    cand_user = with_ends(jax.random.randint(own_keys[3], (CANDS,), 0, USERS), jax.random.fold_in(own_keys[3], 1), 0, USERS - 1).astype(jnp.int32)
    w_in = draw_w_in(jax.random.fold_in(key_list[6], 71), part)
    w_out = noise(key_list[5], (LAYERS, D, D), D ** -0.5, 0.1875)
    return {"history": history, "candidates": candidates, "lengths": lengths, "cand_user": cand_user, "w_in": w_in, "w_out": w_out}


eps = 1e-06

def layer_norm(rows):
    centred = rows - lax.optimization_barrier(jnp.mean(rows, axis=-1, keepdims=True))
    return centred * lax.rsqrt(lax.optimization_barrier(jnp.mean(centred * centred, axis=-1, keepdims=True)) + eps)

def segment_of(positions, ends):
    return lax.optimization_barrier(jnp.sum((positions[:, None] >= ends[None, :]).astype(jnp.int32), axis=1)).astype(jnp.int32)

def reference(history, candidates, lengths, cand_user, w_in, w_out):
    ends = jnp.cumsum(lengths).astype(jnp.int32)
    scale = HEAD_DIM ** (-0.5)
    width = WIN * TOK_DEV
    x_rows = history
    c_rows = candidates
    all_seg = segment_of(jnp.arange(HIST, dtype=jnp.int32), ends)
    for layer in range(LAYERS):
        normed = layer_norm(x_rows.astype(jnp.float32)).astype(jnp.bfloat16)
        proj = jax.nn.silu(jnp.dot(normed, w_in[layer], preferred_element_type=jnp.float32)).astype(jnp.bfloat16)
        u_all = proj[:, 0:D]
        v_all = proj[:, D:2 * D]
        q_all = proj[:, 2 * D:3 * D]
        k_all = proj[:, 3 * D:4 * D]
        front = jnp.zeros(((WIN - 1) * TOK_DEV, D), jnp.bfloat16)
        k_pad = jnp.concatenate([front, k_all], axis=0)
        v_pad = jnp.concatenate([front, v_all], axis=0)

        def hist_block(block):
            first = (block * TOK_DEV).astype(jnp.int32)
            q_blk = lax.dynamic_slice_in_dim(q_all, first, TOK_DEV, 0).astype(jnp.float32).reshape(TOK_DEV, HEADS, HEAD_DIM)
            k_blk = lax.dynamic_slice_in_dim(k_pad, first, width, 0).astype(jnp.float32).reshape(width, HEADS, HEAD_DIM)
            v_blk = lax.dynamic_slice_in_dim(v_pad, first, width, 0).astype(jnp.float32).reshape(width, HEADS, HEAD_DIM)
            q_pos = first + jnp.arange(TOK_DEV, dtype=jnp.int32)
            k_pos = first - (WIN - 1) * TOK_DEV + jnp.arange(width, dtype=jnp.int32)
            allowed = (k_pos[None, :] >= 0) & (k_pos[None, :] <= q_pos[:, None])
            allowed = allowed & (q_pos[:, None] - k_pos[None, :] < SPAN)
            allowed = allowed & (segment_of(k_pos, ends)[None, :] == segment_of(q_pos, ends)[:, None])
            scores = jnp.einsum('qhd,khd->hqk', q_blk, k_blk) * scale
            weight = jnp.where(allowed[None], jax.nn.silu(scores), 0.0).astype(jnp.bfloat16)
            return jnp.einsum('hqk,khd->qhd', weight.astype(jnp.float32), v_blk).reshape(TOK_DEV, D)
        attn = lax.map(hist_block, jnp.arange(N_SEQ, dtype=jnp.int32)).reshape(HIST, D)
        y_rows = (layer_norm(attn) * u_all.astype(jnp.float32)).astype(jnp.bfloat16)
        x_rows = (x_rows.astype(jnp.float32) + jnp.dot(y_rows, w_out[layer], preferred_element_type=jnp.float32)).astype(jnp.bfloat16)
        cnormed = layer_norm(c_rows.astype(jnp.float32)).astype(jnp.bfloat16)
        u_c = jax.nn.silu(jnp.dot(cnormed, w_in[layer][:, 0:D], preferred_element_type=jnp.float32)).astype(jnp.bfloat16)
        q_c = jax.nn.silu(jnp.dot(cnormed, w_in[layer][:, 2 * D:3 * D], preferred_element_type=jnp.float32)).astype(jnp.bfloat16)
        cq_heads = q_c.astype(jnp.float32).reshape(CANDS, HEADS, HEAD_DIM)

        def cand_shard(block, total):
            first = (block * TOK_DEV).astype(jnp.int32)
            k_blk = lax.dynamic_slice_in_dim(k_all, first, TOK_DEV, 0).astype(jnp.float32).reshape(TOK_DEV, HEADS, HEAD_DIM)
            v_blk = lax.dynamic_slice_in_dim(v_all, first, TOK_DEV, 0).astype(jnp.float32).reshape(TOK_DEV, HEADS, HEAD_DIM)
            k_seg = lax.dynamic_slice_in_dim(all_seg, first, TOK_DEV, 0)
            owned = cand_user[:, None] == k_seg[None, :]
            scores = jnp.einsum('chd,khd->hck', cq_heads, k_blk) * scale
            weight = jnp.where(owned[None], jax.nn.silu(scores), 0.0).astype(jnp.bfloat16)
            return total + jnp.einsum('hck,khd->chd', weight.astype(jnp.float32), v_blk).reshape(CANDS, D)
        cattn = lax.fori_loop(0, N_SEQ, cand_shard, jnp.zeros((CANDS, D), jnp.float32))
        y_c = (layer_norm(cattn) * u_c.astype(jnp.float32)).astype(jnp.bfloat16)
        c_rows = (c_rows.astype(jnp.float32) + jnp.dot(y_c, w_out[layer], preferred_element_type=jnp.float32)).astype(jnp.bfloat16)
    return (x_rows, c_rows)
```

```python
import functools

import jax
import jax.numpy as jnp
from jax import lax
from jax.experimental import pallas as pl
from jax.experimental.pallas import tpu as pltpu
from jax.sharding import PartitionSpec as P

HEADS = 8
WIN = 8
STAGES = 4
PREV = WIN - 1
SLOTS = 16
OWN = SLOTS - 1
EPS = 1e-06
BIG = 2.0**30
MESH = pl.DeviceIdType.MESH
F32 = jnp.float32
BF16 = jnp.bfloat16


def silu(s):
    h = 0.5 * s
    return h * jnp.tanh(h) + h


def layer_norm(rows):
    centred = rows - jnp.mean(rows, axis=-1, keepdims=True)
    return centred * lax.rsqrt(jnp.mean(centred * centred, axis=-1, keepdims=True) + EPS)


def contract_last(a, b):
    return lax.dot_general(a, b, (((1,), (1,)), ((), ())), preferred_element_type=F32)


def kernel(
    nz,
    lens,
    users,
    cand,
    hist,
    w_in,
    w_out,
    x_out,
    c_out,
    w,
    wo,
    xv,
    nv,
    uv,
    yv,
    snd,
    kbuf,
    vbuf,
    qbuf,
    kext,
    qext,
    qc_s,
    qcz,
    us_s,
    usr,
    part,
    rs_s,
    rs_r,
    at_s,
    at_r,
    cat_s,
    cat_r,
    w_sem,
    wo_sem,
    x_sem,
    kv_ss,
    kv_rs,
    fw_ss,
    fw_rs,
    q_ss,
    q_rs,
    qc_ss,
    qc_rs,
    us_ss,
    us_rs,
    qg_ss,
    qg_rs,
    ug_ss,
    ug_rs,
    rs_ss,
    rs_rs,
    at_ss,
    at_rs,
    cat_ss,
    cat_rs,
):
    rows, width = xv.shape
    n_cand = cand.shape[0]
    head_dim = width // HEADS
    n_users = lens.shape[0]
    blocks = w.shape[0] // 4
    bw = w.shape[2]
    me = lax.axis_index("seq")
    z = me // HEADS
    r = lax.rem(me, HEADS)
    chip = r // 2

    def in_row(h):
        return {"seq": z * HEADS + h}

    def along(step):
        return {"seq": lax.rem(z + step + nz, nz) * HEADS + r}

    def remote(src, dst, ss, rs, to):
        return pltpu.make_async_remote_copy(
            src_ref=src, dst_ref=dst, send_sem=ss, recv_sem=rs, device_id=to, device_id_type=MESH
        )

    x_copy = pltpu.make_async_copy(hist, xv, x_sem)
    x_copy.start()

    def w_copy(m, b):
        i = m * blocks + b
        return pltpu.make_async_copy(
            w_in.at[0, :, pl.ds(m * width + b * bw, bw)], w.at[i], w_sem.at[i]
        )

    for m in (2, 3, 1, 0):
        for b in range(blocks):
            w_copy(m, b).start()
    wo_copy = pltpu.make_async_copy(w_out.at[0], wo, wo_sem)
    wo_copy.start()

    barrier = pltpu.get_barrier_semaphore()
    for d in range(1, HEADS):
        pl.semaphore_signal(
            barrier, inc=1, device_id=in_row(lax.rem(r + d, HEADS)), device_id_type=MESH
        )
    for step in (-2, -1, 1, 2):
        pl.semaphore_signal(barrier, inc=1, device_id=along(step), device_id_type=MESH)

    lane = lax.broadcasted_iota(jnp.int32, (rows, head_dim), 1)
    row_id = lax.broadcasted_iota(jnp.int32, (rows, head_dim), 0)
    total = nz * HEADS * rows

    def ext_body(kk, carry):
        first = lax.rem((z * HEADS - PREV + kk) * rows + total, total)
        pos = first + row_id
        seg = jnp.zeros((rows, head_dim), jnp.int32)
        end = jnp.int32(0)
        for u in range(n_users):
            end = end + lens[u]
            seg = seg + jnp.where(pos >= end, 1, 0)
        mine = lane == seg
        kext[kk] = jnp.where(mine, 0.0, -BIG).astype(BF16)

        @pl.when(kk >= PREV)
        def _():
            qext[jnp.maximum(kk - PREV, 0)] = jnp.where(mine, 1.0, 0.0).astype(BF16)

        return carry

    lax.fori_loop(0, PREV + HEADS, ext_body, 0)

    pl.semaphore_wait(barrier, HEADS - 1 + 4)

    scale = 0.5 * head_dim ** (-0.5)
    cnormed = layer_norm(cand[...].astype(F32)).astype(BF16)
    per = bw // head_dim
    for b in range(blocks):
        w_copy(2, b).wait()
        qc = silu(jnp.dot(cnormed, w[2 * blocks + b], preferred_element_type=F32)) * scale
        for i in range(per):
            qc_s[b * per + i] = qc[:, i * head_dim : (i + 1) * head_dim].astype(BF16)
    lane_row = lax.broadcasted_iota(jnp.int32, (1, head_dim), 1)
    user_row = jnp.zeros((1, head_dim), F32)
    for i in range(n_cand):
        user_row = jnp.where(lane_row == i, users[i].astype(F32), user_row)
    us_s[0] = user_row

    def qc_copy(d):
        h = lax.rem(r + d, HEADS)
        return remote(qc_s.at[h], qcz.at[OWN, r], qc_ss.at[d], qc_rs.at[d], in_row(h))

    def us_copy(d):
        h = lax.rem(r + d, HEADS)
        return remote(us_s.at[0], usr.at[OWN, r], us_ss.at[d], us_rs.at[d], in_row(h))

    def qc_arrival(d):
        j = lax.rem(r - d + HEADS, HEADS)
        return remote(qc_s.at[j], qcz.at[OWN, j], qc_ss.at[d], qc_rs.at[d], in_row(j))

    def us_arrival(d):
        j = lax.rem(r - d + HEADS, HEADS)
        return remote(us_s.at[0], usr.at[OWN, j], us_ss.at[d], us_rs.at[d], in_row(j))

    for d in range(1, HEADS):
        qc_copy(d).start()
        us_copy(d).start()
    qcz[OWN, r] = qc_s[r]
    usr[OWN, r] = us_s[0]

    x_copy.wait()

    def norm_body(i, carry):
        part_rows = pl.ds(pl.multiple_of(i * 64, 64), 64)
        nv[part_rows, :] = layer_norm(xv[part_rows, :].astype(F32)).astype(BF16)
        return carry

    lax.fori_loop(0, rows // 64, norm_body, 0)

    bufs = (kbuf, vbuf, qbuf)

    def row_copy(m, h):
        if m == 2:
            return remote(snd.at[m, h], qbuf.at[r], q_ss.at[h], q_rs.at[r], in_row(h))
        return remote(
            snd.at[m, h], bufs[m].at[PREV + r], kv_ss.at[m, h], kv_rs.at[m, r], in_row(h)
        )

    def row_arrival(m, j):
        if m == 2:
            return remote(snd.at[m, j], qbuf.at[j], q_ss.at[j], q_rs.at[j], in_row(j))
        return remote(
            snd.at[m, j], bufs[m].at[PREV + j], kv_ss.at[m, j], kv_rs.at[m, j], in_row(j)
        )

    def project(m, source):
        if m != 2:
            for b in range(blocks):
                w_copy(source, b).wait()

        def body(i, carry):
            b = lax.rem(chip + i + 1, blocks)
            p = silu(jnp.dot(nv[...], w[source * blocks + b], preferred_element_type=F32))
            if m == 2:
                p = p * scale
            for i2 in range(per):
                h = b * per + i2
                snd[m, h] = p[:, i2 * head_dim : (i2 + 1) * head_dim].astype(BF16)

                @pl.when(h != r)
                def _():
                    row_copy(m, h).start()

            return carry

        lax.fori_loop(0, blocks, body, 0)

    project(0, 3)
    project(1, 1)
    kbuf[PREV + r] = snd[0, r]
    vbuf[PREV + r] = snd[1, r]

    def gather_pairs(stage):
        ahead = OWN if stage == 1 else 2 * stage - 3
        behind = OWN if stage == 1 else 5 + 2 * stage
        pairs = [(ahead, 2 * stage - 1, 2), (ahead, 2 * stage - 2, 1)]
        if stage < STAGES:
            pairs.append((behind, 7 + 2 * stage, -2))
        pairs.append((behind, 6 + 2 * stage, -1))
        return pairs

    def gather_copies(stage):
        for src, dst, step in gather_pairs(stage):
            yield remote(qcz.at[src], qcz.at[dst], qg_ss.at[dst], qg_rs.at[dst], along(step))
            yield remote(usr.at[src], usr.at[dst], ug_ss.at[dst], ug_rs.at[dst], along(step))

    for d in range(1, HEADS):
        qc_arrival(d).wait_recv()
        us_arrival(d).wait_recv()
    for copy in gather_copies(1):
        copy.start()

    project(2, 2)
    qbuf[r] = snd[2, r]

    for b in range(blocks):
        w_copy(0, b).wait()
        u = silu(jnp.dot(nv[...], w[b], preferred_element_type=F32))
        uv[:, b * bw : (b + 1) * bw] = u.astype(BF16)

    def forward(m, j):
        to = jnp.maximum(j - 1, 0)
        return remote(
            bufs[m].at[PREV + j], bufs[m].at[to], fw_ss.at[m, to], fw_rs.at[m, to], along(1)
        )

    def forward_arrival(m, kk):
        return remote(
            bufs[m].at[PREV + kk + 1], bufs[m].at[kk], fw_ss.at[m, kk], fw_rs.at[m, kk], along(1)
        )

    def forward_all(m):
        @pl.when(r >= 1)
        def _():
            forward(m, r).start()

        def body(i, carry):
            d = i + 1
            j = lax.rem(r - d + HEADS, HEADS)
            row_arrival(m, j).wait_recv()

            @pl.when(j >= 1)
            def _():
                forward(m, j).start()

            return carry

        lax.fori_loop(0, HEADS - 1, body, 0)

    def gather_step(stage):
        for copy in gather_copies(stage - 1):
            copy.wait_recv()
        if stage <= STAGES:
            for copy in gather_copies(stage):
                copy.start()

    forward_all(0)
    gather_step(2)
    forward_all(1)
    gather_step(3)

    slot_lane = lax.broadcasted_iota(jnp.int32, (2 * HEADS * n_cand, head_dim), 1)
    slot_row = lax.broadcasted_iota(jnp.int32, (2 * HEADS * n_cand, head_dim), 0)

    def key_block(kk):
        return jnp.concatenate([kbuf[kk], kext[kk]], axis=1)

    def score(g):
        q = qcz[pl.ds(2 * g, 2)].reshape(2 * HEADS * n_cand, head_dim)
        named = jnp.concatenate(
            [
                jnp.broadcast_to(usr[2 * g + a, j], (n_cand, head_dim))
                for a in range(2)
                for j in range(HEADS)
            ],
            axis=0,
        )
        picked = jnp.where(slot_lane == lax.rem(slot_row, n_cand), named, 0.0)
        user = jnp.sum(picked, axis=1, keepdims=True).astype(jnp.int32)
        ext = jnp.where(slot_lane == user, 1.0, 0.0).astype(BF16)
        qx = jnp.concatenate([q, ext], axis=1)
        acc = jnp.zeros((2 * HEADS * n_cand, head_dim), F32)
        for j in range(HEADS):
            h = contract_last(qx, key_block(PREV + j))
            weight = (h * jnp.tanh(h) + h).astype(BF16)
            acc = acc + jnp.dot(weight, vbuf[PREV + j], preferred_element_type=F32)
        part[pl.ds(2 * g, 2)] = acc.reshape(2, HEADS * n_cand, head_dim)

    def rs_copy(i, step):
        return remote(rs_s.at[i], rs_r.at[i], rs_ss.at[i], rs_rs.at[i], along(step))

    def odd_sends(stage):
        k = STAGES - stage
        rs_s[4 + k] = part[2 * stage - 2].astype(BF16)
        rs_copy(4 + k, -1).start()
        rs_s[12 + k] = part[6 + 2 * stage].astype(BF16)
        rs_copy(12 + k, 1).start()

    def score_stage(stage):
        def body(i, carry):
            score(stage - 1 + STAGES * i)
            return carry

        lax.fori_loop(0, 2, body, 0)
        odd_sends(stage)

    score_stage(1)
    gather_step(4)
    score_stage(2)
    score_stage(3)
    gather_step(5)
    score_stage(4)

    def arrived(stage):
        k = stage - 1
        low = rs_r[k].astype(F32) + rs_r[4 + k].astype(F32)
        high = rs_r[12 + k].astype(F32)
        if stage > 1:
            high = high + rs_r[8 + k].astype(F32)
        return low, high

    def rs_wait(stage):
        k = stage - 1
        rs_copy(k, -2).wait_recv()
        rs_copy(4 + k, -1).wait_recv()
        if stage > 1:
            rs_copy(8 + k, 2).wait_recv()
        rs_copy(12 + k, 1).wait_recv()

    def rs_step(stage):
        k = stage - 1
        e = 2 * WIN // 2 + 2 - 2 * stage
        if stage == 1:
            rs_s[k] = part[e - 1].astype(BF16)
        else:
            rs_wait(stage - 1)
            low, high = arrived(stage - 1)
            rs_s[k] = (part[e - 1] + low).astype(BF16)
            rs_s[8 + k] = (part[7 + e] + high).astype(BF16)
            rs_copy(8 + k, 2).start()
        rs_copy(k, -2).start()

    tri_row = lax.broadcasted_iota(jnp.int32, (rows, rows), 0)
    tri_col = lax.broadcasted_iota(jnp.int32, (rows, rows), 1)

    def at_copy(j):
        return remote(at_s.at[j], at_r.at[r], at_ss.at[j], at_rs.at[r], in_row(j))

    def at_arrival(j):
        return remote(at_s.at[j], at_r.at[j], at_ss.at[j], at_rs.at[j], in_row(j))

    def attend(i, carry):
        j = HEADS - 1 - i

        @pl.when(j < PREV)
        def _():
            forward_arrival(0, jnp.minimum(j, PREV - 1)).wait_recv()
            forward_arrival(1, jnp.minimum(j, PREV - 1)).wait_recv()

        @pl.when(j != r)
        def _():
            row_arrival(2, j).wait_recv()

        qx = jnp.concatenate([qbuf[j], qext[j]], axis=1)
        acc = jnp.zeros((rows, head_dim), F32)
        for t in range(WIN):
            h = contract_last(qx, key_block(j + t))
            if t == 0:
                h = jnp.where(tri_col > tri_row, h, -BIG)
            if t == WIN - 1:
                h = jnp.where(tri_col <= tri_row, h, -BIG)
            weight = (h * jnp.tanh(h) + h).astype(BF16)
            acc = acc + jnp.dot(weight, vbuf[j + t], preferred_element_type=F32)
        at_s[j] = acc.astype(BF16)

        @pl.when(j != r)
        def _():
            at_copy(j).start()

        return carry

    rs_step(1)
    lax.fori_loop(0, HEADS // 2, attend, 0)
    rs_step(2)
    lax.fori_loop(HEADS // 2, HEADS, attend, 0)
    at_r[r] = at_s[r]
    rs_step(3)

    def at_wait(i, carry):
        at_arrival(lax.rem(r + i + 1, HEADS)).wait_recv()
        return carry

    lax.fori_loop(0, HEADS - 1, at_wait, 0)

    def y_body(i, carry):
        part_rows = pl.ds(pl.multiple_of(i * 64, 64), 64)
        a = jnp.concatenate([at_r[h, part_rows, :] for h in range(HEADS)], axis=1)
        y = layer_norm(a.astype(F32)) * uv[part_rows, :].astype(F32)
        yv[part_rows, :] = y.astype(BF16)
        return carry

    lax.fori_loop(0, rows // 64, y_body, 0)
    wo_copy.wait()
    for b in range(width // 256):
        cols = slice(b * 256, (b + 1) * 256)
        o = jnp.dot(yv[...], wo[:, cols], preferred_element_type=F32)
        x_out[:, cols] = (xv[:, cols].astype(F32) + o).astype(BF16)

    rs_step(4)
    u_c = jnp.concatenate(
        [
            silu(jnp.dot(cnormed, w[b], preferred_element_type=F32)).astype(BF16)
            for b in range(blocks)
        ],
        axis=1,
    ).astype(F32)
    rs_wait(4)
    low, high = arrived(4)
    cat_s[...] = (part[OWN] + low + high).reshape(HEADS, n_cand, head_dim)

    def cat_copy(d):
        h = lax.rem(r + d, HEADS)
        return remote(cat_s.at[h], cat_r.at[r], cat_ss.at[d], cat_rs.at[d], in_row(h))

    def cat_arrival(d):
        j = lax.rem(r - d + HEADS, HEADS)
        return remote(cat_s.at[j], cat_r.at[j], cat_ss.at[d], cat_rs.at[d], in_row(j))

    for d in range(1, HEADS):
        cat_copy(d).start()
    cat_r[r] = cat_s[r]
    for d in range(1, HEADS):
        cat_arrival(d).wait_recv()
    a = jnp.concatenate([cat_r[h] for h in range(HEADS)], axis=1)
    y_c = (layer_norm(a) * u_c).astype(BF16)
    o = jnp.dot(y_c, wo[...], preferred_element_type=F32)
    c_out[...] = (cand[...].astype(F32) + o).astype(BF16)

    for d in range(1, HEADS):
        qc_copy(d).wait_send()
        us_copy(d).wait_send()
        cat_copy(d).wait_send()
    for stage in range(1, STAGES + 1):
        for copy in gather_copies(stage):
            copy.wait_send()
        k = stage - 1
        rs_copy(k, -2).wait_send()
        rs_copy(4 + k, -1).wait_send()
        if stage > 1:
            rs_copy(8 + k, 2).wait_send()
        rs_copy(12 + k, 1).wait_send()

    def drain(i, carry):
        h = lax.rem(r + i + 1, HEADS)
        for m in range(3):
            row_copy(m, h).wait_send()
        at_copy(h).wait_send()
        forward(0, i + 1).wait_send()
        forward(1, i + 1).wait_send()
        return carry

    lax.fori_loop(0, HEADS - 1, drain, 0)


def per_device(nz, history, candidates, lengths, cand_user, w_in, w_out):
    rows, width = history.shape
    n_cand = candidates.shape[0]
    hd = width // HEADS
    bw = 256
    dma = pltpu.SemaphoreType.DMA
    vmem = pl.BlockSpec(memory_space=pltpu.VMEM)
    smem = pl.BlockSpec(memory_space=pltpu.SMEM)
    hbm = pl.BlockSpec(memory_space=pl.ANY)
    shards = PREV + HEADS
    scratch = [
        pltpu.VMEM((4 * width // bw, width, bw), BF16),
        pltpu.VMEM((width, width), BF16),
        pltpu.VMEM((rows, width), BF16),
        pltpu.VMEM((rows, width), BF16),
        pltpu.VMEM((rows, width), BF16),
        pltpu.VMEM((rows, width), BF16),
        pltpu.VMEM((3, HEADS, rows, hd), BF16),
        pltpu.VMEM((shards, rows, hd), BF16),
        pltpu.VMEM((shards, rows, hd), BF16),
        pltpu.VMEM((HEADS, rows, hd), BF16),
        pltpu.VMEM((shards, rows, hd), BF16),
        pltpu.VMEM((HEADS, rows, hd), BF16),
        pltpu.VMEM((HEADS, n_cand, hd), BF16),
        pltpu.VMEM((SLOTS, HEADS, n_cand, hd), BF16),
        pltpu.VMEM((1, 1, hd), F32),
        pltpu.VMEM((SLOTS, HEADS, 1, hd), F32),
        pltpu.VMEM((SLOTS, HEADS * n_cand, hd), F32),
        pltpu.VMEM((SLOTS, HEADS * n_cand, hd), BF16),
        pltpu.VMEM((SLOTS, HEADS * n_cand, hd), BF16),
        pltpu.VMEM((HEADS, rows, hd), BF16),
        pltpu.VMEM((HEADS, rows, hd), BF16),
        pltpu.VMEM((HEADS, n_cand, hd), F32),
        pltpu.VMEM((HEADS, n_cand, hd), F32),
        dma((4 * width // bw,)),
        dma,
        dma,
        dma((2, HEADS)),
        dma((2, HEADS)),
        dma((2, PREV)),
        dma((2, PREV)),
        dma((HEADS,)),
        dma((HEADS,)),
        dma((HEADS,)),
        dma((HEADS,)),
        dma((HEADS,)),
        dma((HEADS,)),
        dma((SLOTS,)),
        dma((SLOTS,)),
        dma((SLOTS,)),
        dma((SLOTS,)),
        dma((SLOTS,)),
        dma((SLOTS,)),
        dma((HEADS,)),
        dma((HEADS,)),
        dma((HEADS,)),
        dma((HEADS,)),
    ]
    return pl.pallas_call(
        functools.partial(kernel, nz),
        out_shape=(
            jax.ShapeDtypeStruct(history.shape, BF16),
            jax.ShapeDtypeStruct(candidates.shape, BF16),
        ),
        in_specs=[smem, smem, vmem, hbm, hbm, hbm],
        out_specs=(vmem, vmem),
        scratch_shapes=scratch,
        compiler_params=pltpu.CompilerParams(
            collective_id=0, has_side_effects=True, vmem_limit_bytes=60 * 2**20
        ),
    )(lengths, cand_user, candidates, history, w_in, w_out)


def solution(mesh):
    nz = mesh.shape["seq"] // HEADS
    both = ("grp", "seq")
    return jax.shard_map(
        functools.partial(per_device, nz),
        mesh=mesh,
        in_specs=(P(both, None), P(both, None), P("grp"), P(both), P(), P()),
        out_specs=(P(both, None), P(both, None)),
        check_vma=False,
    )
```

```python
import functools

import jax
import jax.numpy as jnp
from jax import lax
from jax.experimental import pallas as pl
from jax.experimental.pallas import tpu as pltpu
from jax.sharding import PartitionSpec as P

HEADS = 8
WIN = 8
STAGES = 4
PREV = WIN - 1
SLOTS = 16
OWN = SLOTS - 1
EPS = 1e-06
BIG = 2.0**30
MESH = pl.DeviceIdType.MESH
F32 = jnp.float32
BF16 = jnp.bfloat16


def silu(s):
    h = 0.5 * s
    return h * jnp.tanh(h) + h


def layer_norm(rows):
    centred = rows - jnp.mean(rows, axis=-1, keepdims=True)
    return centred * lax.rsqrt(jnp.mean(centred * centred, axis=-1, keepdims=True) + EPS)


def contract_last(a, b):
    return lax.dot_general(a, b, (((1,), (1,)), ((), ())), preferred_element_type=F32)


def kernel(
    nz,
    lens,
    users,
    cand,
    hist,
    w_in,
    w_out,
    x_out,
    c_out,
    w,
    wo,
    xv,
    nv,
    uv,
    yv,
    snd,
    kbuf,
    vbuf,
    qbuf,
    qnbuf,
    kext,
    qext,
    qnext,
    qc_s,
    qcz,
    us_s,
    usr,
    part,
    rs_s,
    rs_r,
    at_s,
    at_r,
    an_s,
    an_r,
    cat_s,
    cat_r,
    w_sem,
    wo_sem,
    x_sem,
    kv_ss,
    kv_rs,
    q_ss,
    q_rs,
    qn_ss,
    qn_rs,
    qc_ss,
    qc_rs,
    us_ss,
    us_rs,
    qg_ss,
    qg_rs,
    ug_ss,
    ug_rs,
    rs_ss,
    rs_rs,
    at_ss,
    at_rs,
    an_ss,
    an_rs,
    cat_ss,
    cat_rs,
):
    rows, width = xv.shape
    n_cand = cand.shape[0]
    head_dim = width // HEADS
    n_users = lens.shape[0]
    blocks = w.shape[0] // 4
    bw = w.shape[2]
    me = lax.axis_index("seq")
    z = me // HEADS
    r = lax.rem(me, HEADS)
    chip = r // 2

    def in_row(h):
        return {"seq": z * HEADS + h}

    def in_rows(step, h):
        return {"seq": lax.rem(z + step + nz, nz) * HEADS + h}

    def along(step):
        return in_rows(step, r)

    def remote(src, dst, ss, rs, to):
        return pltpu.make_async_remote_copy(
            src_ref=src, dst_ref=dst, send_sem=ss, recv_sem=rs, device_id=to, device_id_type=MESH
        )

    x_copy = pltpu.make_async_copy(hist, xv, x_sem)

    def w_copy(m, b):
        i = m * blocks + b
        return pltpu.make_async_copy(
            w_in.at[0, :, pl.ds(m * width + b * bw, bw)], w.at[i], w_sem.at[i]
        )

    for b in range(blocks):
        w_copy(2, b).start()
    x_copy.start()
    wo_copy = pltpu.make_async_copy(w_out.at[0], wo, wo_sem)

    barrier = pltpu.get_barrier_semaphore()
    for d in range(1, HEADS):
        pl.semaphore_signal(
            barrier, inc=1, device_id=in_row(lax.rem(r + d, HEADS)), device_id_type=MESH
        )
    for step in (-2, 2):
        pl.semaphore_signal(barrier, inc=1, device_id=along(step), device_id_type=MESH)
    for step in (-1, 1):
        for h in range(HEADS):
            pl.semaphore_signal(barrier, inc=1, device_id=in_rows(step, h), device_id_type=MESH)

    pl.semaphore_wait(barrier, HEADS - 1 + 2 + 2 * HEADS)

    scale = 0.5 * head_dim ** (-0.5)
    cnormed = layer_norm(cand[...].astype(F32)).astype(BF16)
    per = bw // head_dim
    for b in range(blocks):
        w_copy(2, b).wait()
        qc = silu(jnp.dot(cnormed, w[2 * blocks + b], preferred_element_type=F32)) * scale
        for i in range(per):
            qc_s[b * per + i] = qc[:, i * head_dim : (i + 1) * head_dim].astype(BF16)
    for m in (3, 1, 0):
        for b in range(blocks):
            w_copy(m, b).start()
    wo_copy.start()
    lane_row = lax.broadcasted_iota(jnp.int32, (1, head_dim), 1)
    user_row = jnp.zeros((1, head_dim), F32)
    for i in range(n_cand):
        user_row = jnp.where(lane_row == i, users[i].astype(F32), user_row)
    us_s[0] = user_row

    def qc_copy(d):
        h = lax.rem(r + d, HEADS)
        return remote(qc_s.at[h], qcz.at[OWN, r], qc_ss.at[d], qc_rs.at[d], in_row(h))

    def us_copy(d):
        h = lax.rem(r + d, HEADS)
        return remote(us_s.at[0], usr.at[OWN, r], us_ss.at[d], us_rs.at[d], in_row(h))

    def qc_arrival(d):
        j = lax.rem(r - d + HEADS, HEADS)
        return remote(qc_s.at[j], qcz.at[OWN, j], qc_ss.at[d], qc_rs.at[d], in_row(j))

    def us_arrival(d):
        j = lax.rem(r - d + HEADS, HEADS)
        return remote(us_s.at[0], usr.at[OWN, j], us_ss.at[d], us_rs.at[d], in_row(j))

    for d in range(1, HEADS):
        qc_copy(d).start()
        us_copy(d).start()
    qcz[OWN, r] = qc_s[r]
    usr[OWN, r] = us_s[0]

    x_copy.wait()

    def norm_body(i, carry):
        part_rows = pl.ds(pl.multiple_of(i * 64, 64), 64)
        nv[part_rows, :] = layer_norm(xv[part_rows, :].astype(F32)).astype(BF16)
        return carry

    lax.fori_loop(0, rows // 64, norm_body, 0)
    bufs = (kbuf, vbuf, qbuf)

    def row_copy(m, h):
        if m == 2:
            return remote(snd.at[m, h], qbuf.at[r], q_ss.at[h], q_rs.at[r], in_row(h))
        return remote(
            snd.at[m, h], bufs[m].at[r], kv_ss.at[m, h], kv_rs.at[m, r], in_row(h)
        )

    def row_arrival(m, j):
        if m == 2:
            return remote(snd.at[m, j], qbuf.at[j], q_ss.at[j], q_rs.at[j], in_row(j))
        return remote(
            snd.at[m, j], bufs[m].at[j], kv_ss.at[m, j], kv_rs.at[m, j], in_row(j)
        )

    def project(m, source):
        if m != 2:
            for b in range(blocks):
                w_copy(source, b).wait()

        def body(i, carry):
            b = lax.rem(chip + i + 1, blocks)
            p = silu(jnp.dot(nv[...], w[source * blocks + b], preferred_element_type=F32))
            if m == 2:
                p = p * scale
            for i2 in range(per):
                h = b * per + i2
                snd[m, h] = p[:, i2 * head_dim : (i2 + 1) * head_dim].astype(BF16)

                @pl.when(h != r)
                def _():
                    row_copy(m, h).start()

            return carry

        lax.fori_loop(0, blocks, body, 0)

    project(0, 3)
    kbuf[r] = snd[0, r]

    def gather_pairs(stage):
        ahead = OWN if stage == 1 else 2 * stage - 3
        behind = OWN if stage == 1 else 5 + 2 * stage
        pairs = [(ahead, 2 * stage - 1, 2), (ahead, 2 * stage - 2, 1)]
        if stage < STAGES:
            pairs.append((behind, 7 + 2 * stage, -2))
        pairs.append((behind, 6 + 2 * stage, -1))
        return pairs

    def gather_copies(stage):
        for src, dst, step in gather_pairs(stage):
            yield remote(qcz.at[src], qcz.at[dst], qg_ss.at[dst], qg_rs.at[dst], along(step))
            yield remote(usr.at[src], usr.at[dst], ug_ss.at[dst], ug_rs.at[dst], along(step))

    for d in range(1, HEADS):
        qc_arrival(d).wait_recv()
        us_arrival(d).wait_recv()
    for copy in gather_copies(1):
        copy.start()

    project(1, 1)
    vbuf[r] = snd[1, r]
    project(2, 2)
    qbuf[r] = snd[2, r]

    def qn_copy(h):
        return remote(snd.at[2, h], qnbuf.at[r], qn_ss.at[h], qn_rs.at[r], in_rows(-1, h))

    def qn_arrival(j):
        return remote(snd.at[2, j], qnbuf.at[j], qn_ss.at[j], qn_rs.at[j], in_rows(1, j))

    def qn_sends(first):
        @pl.when(r < PREV)
        def _():
            for i in (first, first + 1):
                qn_copy(lax.rem(r + i + 1, HEADS)).start()

    lane = lax.broadcasted_iota(jnp.int32, (rows, head_dim), 1)
    row_id = lax.broadcasted_iota(jnp.int32, (rows, head_dim), 0)
    total = nz * HEADS * rows

    def owner(j):
        pos = lax.rem((z * HEADS + j) * rows, total) + row_id
        seg = jnp.zeros((rows, head_dim), jnp.int32)
        end = jnp.int32(0)
        for u in range(n_users):
            end = end + lens[u]
            seg = seg + jnp.where(pos >= end, 1, 0)
        return lane == seg

    def ext_body(j, carry):
        mine = owner(j)
        kext[j] = jnp.where(mine, 0.0, -BIG).astype(BF16)
        qext[j] = jnp.where(mine, 1.0, 0.0).astype(BF16)
        qnext[j] = jnp.where(owner(HEADS + j), 1.0, 0.0).astype(BF16)
        return carry

    lax.fori_loop(0, HEADS, ext_body, 0)

    def gather_step(stage):
        for copy in gather_copies(stage - 1):
            copy.wait_recv()
        if stage <= STAGES:
            for copy in gather_copies(stage):
                copy.start()

    gather_step(2)
    qn_sends(0)

    for b in range(blocks):
        w_copy(0, b).wait()
        u = silu(jnp.dot(nv[...], w[b], preferred_element_type=F32))
        uv[:, b * bw : (b + 1) * bw] = u.astype(BF16)

    gather_step(3)
    qn_sends(2)

    def kv_wait(i, carry):
        j = lax.rem(r + i + 1, HEADS)
        row_arrival(0, j).wait_recv()
        row_arrival(1, j).wait_recv()
        return carry

    lax.fori_loop(0, HEADS - 1, kv_wait, 0)

    n_slot = HEADS * n_cand
    slot_lane = lax.broadcasted_iota(jnp.int32, (4 * n_slot, head_dim), 1)
    slot_row = lax.broadcasted_iota(jnp.int32, (4 * n_slot, head_dim), 0)

    def key_block(j):
        return jnp.concatenate([kbuf[j], kext[j]], axis=1)

    def weigh(h):
        return (h * jnp.tanh(h) + h).astype(BF16)

    def score(slots):
        q = jnp.concatenate([qcz[i].reshape(n_slot, head_dim) for i in slots], axis=0)
        named = jnp.concatenate(
            [jnp.broadcast_to(usr[i, j], (n_cand, head_dim)) for i in slots for j in range(HEADS)],
            axis=0,
        )
        picked = jnp.where(slot_lane == lax.rem(slot_row, n_cand), named, 0.0)
        user = jnp.sum(picked, axis=1, keepdims=True).astype(jnp.int32)
        ext = jnp.where(slot_lane == user, 1.0, 0.0).astype(BF16)
        qx = jnp.concatenate([q, ext], axis=1)
        acc = jnp.zeros((4 * n_slot, head_dim), F32)
        for j in range(HEADS):
            weight = weigh(contract_last(qx, key_block(j)))
            acc = acc + jnp.dot(weight, vbuf[j], preferred_element_type=F32)
        for a, i in enumerate(slots):
            part[i] = acc[a * n_slot : (a + 1) * n_slot]

    def rs_copy(i, step):
        return remote(rs_s.at[i], rs_r.at[i], rs_ss.at[i], rs_rs.at[i], along(step))

    def odd_sends(stage):
        k = STAGES - stage
        rs_s[4 + k] = part[2 * stage - 2].astype(BF16)
        rs_copy(4 + k, -1).start()
        rs_s[12 + k] = part[6 + 2 * stage].astype(BF16)
        rs_copy(12 + k, 1).start()

    def score_stage(stage):
        score((2 * stage - 2, 2 * stage - 1, 6 + 2 * stage, 7 + 2 * stage))
        odd_sends(stage)

    score_stage(1)
    gather_step(4)
    qn_sends(4)
    score_stage(2)
    qn_sends(6)
    score_stage(3)
    gather_step(5)
    score_stage(4)

    def arrived(stage):
        k = stage - 1
        low = rs_r[k].astype(F32) + rs_r[4 + k].astype(F32)
        high = rs_r[12 + k].astype(F32)
        if stage > 1:
            high = high + rs_r[8 + k].astype(F32)
        return low, high

    def rs_wait(stage):
        k = stage - 1
        rs_copy(k, -2).wait_recv()
        rs_copy(4 + k, -1).wait_recv()
        if stage > 1:
            rs_copy(8 + k, 2).wait_recv()
        rs_copy(12 + k, 1).wait_recv()

    def rs_step(stage):
        k = stage - 1
        e = 2 * WIN // 2 + 2 - 2 * stage
        if stage == 1:
            rs_s[k] = part[e - 1].astype(BF16)
        else:
            rs_wait(stage - 1)
            low, high = arrived(stage - 1)
            rs_s[k] = (part[e - 1] + low).astype(BF16)
            rs_s[8 + k] = (part[7 + e] + high).astype(BF16)
            rs_copy(8 + k, 2).start()
        rs_copy(k, -2).start()

    one_row = lax.broadcasted_iota(jnp.int32, (rows, rows), 0)
    one_col = lax.broadcasted_iota(jnp.int32, (rows, rows), 1)
    two_row = lax.broadcasted_iota(jnp.int32, (2 * rows, rows), 0)
    two_col = lax.broadcasted_iota(jnp.int32, (2 * rows, rows), 1)

    def at_copy(j):
        return remote(at_s.at[j], at_r.at[r], at_ss.at[j], at_rs.at[r], in_row(j))

    def at_arrival(j):
        return remote(at_s.at[j], at_r.at[j], at_ss.at[j], at_rs.at[j], in_row(j))

    def an_copy(j):
        return remote(an_s.at[j], an_r.at[r], an_ss.at[j], an_rs.at[r], in_rows(1, j))

    def an_arrival(h):
        return remote(an_s.at[0], an_r.at[h], an_ss.at[0], an_rs.at[h], in_rows(-1, h))

    def both(ref, p):
        return ref[2 * p : 2 * p + 2].reshape(2 * rows, head_dim)

    def values(weight, j):
        return jnp.dot(weight, vbuf[j], preferred_element_type=F32)

    def attend_own(p):
        for j in (2 * p, 2 * p + 1):

            @pl.when(j != r)
            def _():
                row_arrival(2, j).wait_recv()

        qx = jnp.concatenate([both(qbuf, p), both(qext, p)], axis=1)
        acc = jnp.zeros((2 * rows, head_dim), F32)
        for j in range(2 * p + 1):
            h = contract_last(qx, key_block(j))
            if j == 2 * p:
                h = jnp.where((two_row >= rows) | (two_col <= two_row), h, -BIG)
            if 2 * p + 1 - j == PREV:
                h = jnp.where((two_row < rows) | (two_col > two_row - rows), h, -BIG)
            acc = acc + values(weigh(h), j)
        h = contract_last(qx[rows:], key_block(2 * p + 1))
        h = jnp.where(one_col <= one_row, h, -BIG)
        at_s[2 * p] = acc[:rows].astype(BF16)
        at_s[2 * p + 1] = (acc[rows:] + values(weigh(h), 2 * p + 1)).astype(BF16)
        for j in (2 * p, 2 * p + 1):

            @pl.when(j != r)
            def _():
                at_copy(j).start()

    def attend_next(p):
        many = 2 * p + 1 < PREV
        qn_arrival(2 * p).wait_recv()
        q = jnp.concatenate([qnbuf[2 * p], qnext[2 * p]], axis=1)
        h = contract_last(q, key_block(2 * p + 1))
        h = jnp.where(one_col > one_row, h, -BIG)
        acc = values(weigh(h), 2 * p + 1)
        if many:
            qn_arrival(2 * p + 1).wait_recv()
            qx = jnp.concatenate([both(qnbuf, p), both(qnext, p)], axis=1)
            more = jnp.zeros((2 * rows, head_dim), F32)
            for j in range(2 * p + 2, HEADS):
                h = contract_last(qx, key_block(j))
                if j == 2 * p + 2:
                    h = jnp.where((two_row < rows) | (two_col > two_row - rows), h, -BIG)
                more = more + values(weigh(h), j)
            acc = acc + more[:rows]
            an_s[2 * p + 1] = more[rows:].astype(BF16)
        an_s[2 * p] = acc.astype(BF16)
        an_copy(2 * p).start()
        if many:
            an_copy(2 * p + 1).start()

    rs_step(1)
    attend_next(0)
    attend_next(1)
    attend_own(0)
    rs_step(2)
    attend_next(2)
    attend_next(3)
    attend_own(1)
    attend_own(2)
    rs_step(3)
    attend_own(3)
    at_r[r] = at_s[r]
    rs_step(4)
    u_c = jnp.concatenate(
        [
            silu(jnp.dot(cnormed, w[b], preferred_element_type=F32)).astype(BF16)
            for b in range(blocks)
        ],
        axis=1,
    ).astype(F32)

    rs_wait(4)
    low, high = arrived(4)
    cat_s[...] = (part[OWN] + low + high).reshape(HEADS, n_cand, head_dim)

    def cat_copy(d):
        h = lax.rem(r + d, HEADS)
        return remote(cat_s.at[h], cat_r.at[r], cat_ss.at[d], cat_rs.at[d], in_row(h))

    def cat_arrival(d):
        j = lax.rem(r - d + HEADS, HEADS)
        return remote(cat_s.at[j], cat_r.at[j], cat_ss.at[d], cat_rs.at[d], in_row(j))

    for d in range(1, HEADS):
        cat_copy(d).start()
    cat_r[r] = cat_s[r]

    def at_wait(i, carry):
        at_arrival(lax.rem(r + i + 1, HEADS)).wait_recv()
        return carry

    lax.fori_loop(0, HEADS - 1, at_wait, 0)

    @pl.when(r < PREV)
    def _():
        for h in range(HEADS):
            an_arrival(h).wait_recv()

    @pl.when(r == PREV)
    def _():
        an_r[...] = jnp.zeros_like(an_r)

    def y_body(i, carry):
        part_rows = pl.ds(pl.multiple_of(i * 64, 64), 64)
        a = jnp.concatenate(
            [
                at_r[h, part_rows, :].astype(F32) + an_r[h, part_rows, :].astype(F32)
                for h in range(HEADS)
            ],
            axis=1,
        )
        y = layer_norm(a) * uv[part_rows, :].astype(F32)
        yv[part_rows, :] = y.astype(BF16)
        return carry

    lax.fori_loop(0, rows // 64, y_body, 0)
    wo_copy.wait()
    for b in range(width // 256):
        cols = slice(b * 256, (b + 1) * 256)
        o = jnp.dot(yv[...], wo[:, cols], preferred_element_type=F32)
        x_out[:, cols] = (xv[:, cols].astype(F32) + o).astype(BF16)

    for d in range(1, HEADS):
        cat_arrival(d).wait_recv()
    a = jnp.concatenate([cat_r[h] for h in range(HEADS)], axis=1)
    y_c = (layer_norm(a) * u_c).astype(BF16)
    o = jnp.dot(y_c, wo[...], preferred_element_type=F32)
    c_out[...] = (cand[...].astype(F32) + o).astype(BF16)

    for d in range(1, HEADS):
        qc_copy(d).wait_send()
        us_copy(d).wait_send()
        cat_copy(d).wait_send()
    for stage in range(1, STAGES + 1):
        for copy in gather_copies(stage):
            copy.wait_send()
        k = stage - 1
        rs_copy(k, -2).wait_send()
        rs_copy(4 + k, -1).wait_send()
        if stage > 1:
            rs_copy(8 + k, 2).wait_send()
        rs_copy(12 + k, 1).wait_send()

    def drain(i, carry):
        h = lax.rem(r + i + 1, HEADS)
        for m in range(3):
            row_copy(m, h).wait_send()
        at_copy(h).wait_send()
        an_copy(i).wait_send()
        return carry

    lax.fori_loop(0, HEADS - 1, drain, 0)

    @pl.when(r < PREV)
    def _():
        for h in range(HEADS):
            qn_copy(h).wait_send()


def per_device(nz, history, candidates, lengths, cand_user, w_in, w_out):
    rows, width = history.shape
    n_cand = candidates.shape[0]
    hd = width // HEADS
    bw = 256
    dma = pltpu.SemaphoreType.DMA
    vmem = pl.BlockSpec(memory_space=pltpu.VMEM)
    smem = pl.BlockSpec(memory_space=pltpu.SMEM)
    hbm = pl.BlockSpec(memory_space=pl.ANY)
    scratch = [
        pltpu.VMEM((4 * width // bw, width, bw), BF16),
        pltpu.VMEM((width, width), BF16),
        pltpu.VMEM((rows, width), BF16),
        pltpu.VMEM((rows, width), BF16),
        pltpu.VMEM((rows, width), BF16),
        pltpu.VMEM((rows, width), BF16),
        pltpu.VMEM((3, HEADS, rows, hd), BF16),
        pltpu.VMEM((HEADS, rows, hd), BF16),
        pltpu.VMEM((HEADS, rows, hd), BF16),
        pltpu.VMEM((HEADS, rows, hd), BF16),
        pltpu.VMEM((HEADS, rows, hd), BF16),
        pltpu.VMEM((HEADS, rows, hd), BF16),
        pltpu.VMEM((HEADS, rows, hd), BF16),
        pltpu.VMEM((HEADS, rows, hd), BF16),
        pltpu.VMEM((HEADS, n_cand, hd), BF16),
        pltpu.VMEM((SLOTS, HEADS, n_cand, hd), BF16),
        pltpu.VMEM((1, 1, hd), F32),
        pltpu.VMEM((SLOTS, HEADS, 1, hd), F32),
        pltpu.VMEM((SLOTS, HEADS * n_cand, hd), F32),
        pltpu.VMEM((SLOTS, HEADS * n_cand, hd), BF16),
        pltpu.VMEM((SLOTS, HEADS * n_cand, hd), BF16),
        pltpu.VMEM((HEADS, rows, hd), BF16),
        pltpu.VMEM((HEADS, rows, hd), BF16),
        pltpu.VMEM((HEADS, rows, hd), BF16),
        pltpu.VMEM((HEADS, rows, hd), BF16),
        pltpu.VMEM((HEADS, n_cand, hd), F32),
        pltpu.VMEM((HEADS, n_cand, hd), F32),
        dma((4 * width // bw,)),
        dma,
        dma,
        dma((2, HEADS)),
        dma((2, HEADS)),
        dma((HEADS,)),
        dma((HEADS,)),
        dma((HEADS,)),
        dma((HEADS,)),
        dma((HEADS,)),
        dma((HEADS,)),
        dma((HEADS,)),
        dma((HEADS,)),
        dma((SLOTS,)),
        dma((SLOTS,)),
        dma((SLOTS,)),
        dma((SLOTS,)),
        dma((SLOTS,)),
        dma((SLOTS,)),
        dma((HEADS,)),
        dma((HEADS,)),
        dma((HEADS,)),
        dma((HEADS,)),
        dma((HEADS,)),
        dma((HEADS,)),
    ]
    return pl.pallas_call(
        functools.partial(kernel, nz),
        out_shape=(
            jax.ShapeDtypeStruct(history.shape, BF16),
            jax.ShapeDtypeStruct(candidates.shape, BF16),
        ),
        in_specs=[smem, smem, vmem, hbm, hbm, hbm],
        out_specs=(vmem, vmem),
        scratch_shapes=scratch,
        compiler_params=pltpu.CompilerParams(
            collective_id=0, has_side_effects=True, vmem_limit_bytes=60 * 2**20
        ),
    )(lengths, cand_user, candidates, history, w_in, w_out)


def solution(mesh):
    nz = mesh.shape["seq"] // HEADS
    both = ("grp", "seq")
    return jax.shard_map(
        functools.partial(per_device, nz),
        mesh=mesh,
        in_specs=(P(both, None), P(both, None), P("grp"), P(both), P(), P()),
        out_specs=(P(both, None), P(both, None)),
        check_vma=False,
    )
```

```python
import functools

import jax
import jax.numpy as jnp
from jax import lax
from jax.experimental import pallas as pl
from jax.experimental.pallas import tpu as pltpu
from jax.sharding import PartitionSpec as P

HEADS = 8
WIN = 8
STAGES = 4
PREV = WIN - 1
SLOTS = 16
OWN = SLOTS - 1
EPS = 1e-06
BIG = 2.0**30
MESH = pl.DeviceIdType.MESH
F32 = jnp.float32
BF16 = jnp.bfloat16


def silu(s):
    h = 0.5 * s
    return h * jnp.tanh(h) + h


def layer_norm(rows):
    centred = rows - jnp.mean(rows, axis=-1, keepdims=True)
    return centred * lax.rsqrt(jnp.mean(centred * centred, axis=-1, keepdims=True) + EPS)


def contract_last(a, b):
    return lax.dot_general(a, b, (((1,), (1,)), ((), ())), preferred_element_type=F32)


def kernel(
    nz,
    lens_in,
    users_in,
    cand_in,
    hist,
    w_in,
    w_out,
    x_out,
    c_out,
    lens,
    users,
    cand,
    w,
    wo,
    xv,
    nv,
    uv,
    yv,
    snd,
    kbuf,
    vbuf,
    qbuf,
    qnbuf,
    kext,
    qext,
    qnext,
    qc_s,
    qcz,
    us_s,
    usr,
    qce,
    part,
    rs_s,
    rs_r,
    at_s,
    at_r,
    an_s,
    an_r,
    cat_s,
    cat_r,
    small_sem,
    w_sem,
    wo_sem,
    x_sem,
    kv_ss,
    kv_rs,
    q_ss,
    q_rs,
    qn_ss,
    qn_rs,
    qc_ss,
    qc_rs,
    us_ss,
    us_rs,
    qg_ss,
    qg_rs,
    ug_ss,
    ug_rs,
    rs_ss,
    rs_rs,
    at_ss,
    at_rs,
    an_ss,
    an_rs,
    cat_ss,
    cat_rs,
):
    rows, width = xv.shape
    n_cand = cand.shape[0]
    head_dim = width // HEADS
    n_users = lens.shape[0]
    blocks = w.shape[0] // 4
    bw = w.shape[2]
    me = lax.axis_index("seq")
    z = me // HEADS
    r = lax.rem(me, HEADS)
    chip = r // 2

    def in_row(h):
        return {"seq": z * HEADS + h}

    def in_rows(step, h):
        return {"seq": lax.rem(z + step + nz, nz) * HEADS + h}

    def along(step):
        return in_rows(step, r)

    def remote(src, dst, ss, rs, to):
        return pltpu.make_async_remote_copy(
            src_ref=src, dst_ref=dst, send_sem=ss, recv_sem=rs, device_id=to, device_id_type=MESH
        )

    small = [
        pltpu.make_async_copy(src, dst, small_sem.at[i])
        for i, (src, dst) in enumerate(((cand_in, cand), (users_in, users), (lens_in, lens)))
    ]
    for copy in small:
        copy.start()
    x_copy = pltpu.make_async_copy(hist, xv, x_sem)

    def w_copy(m, b):
        i = m * blocks + b
        return pltpu.make_async_copy(
            w_in.at[0, :, pl.ds(pl.multiple_of(m * width + b * bw, bw), bw)], w.at[i], w_sem.at[i]
        )

    def block_at(i):
        return lax.rem(chip + i + (i // 2) * (1 - 2 * (i % 2)), blocks)

    for b in range(blocks):
        w_copy(2, b).start()
    x_copy.start()
    wo_copy = pltpu.make_async_copy(w_out.at[0], wo, wo_sem)

    barrier = pltpu.get_barrier_semaphore()
    for d in range(1, HEADS):
        pl.semaphore_signal(
            barrier, inc=1, device_id=in_row(lax.rem(r + d, HEADS)), device_id_type=MESH
        )
    for step in (-2, 2):
        pl.semaphore_signal(barrier, inc=1, device_id=along(step), device_id_type=MESH)
    for step in (-1, 1):
        for h in range(HEADS):
            pl.semaphore_signal(barrier, inc=1, device_id=in_rows(step, h), device_id_type=MESH)

    pl.semaphore_wait(barrier, HEADS - 1 + 2 + 2 * HEADS)
    for i in range(blocks):
        w_copy(3, block_at(i)).start()
        w_copy(1, block_at(i)).start()

    scale = 0.5 * head_dim ** (-0.5)
    for copy in small:
        copy.wait()
    cnormed = layer_norm(cand[...].astype(F32)).astype(BF16)
    per = bw // head_dim
    for b in range(blocks):
        w_copy(2, b).wait()
        qc = silu(jnp.dot(cnormed, w[2 * blocks + b], preferred_element_type=F32)) * scale
        for i in range(per):
            qc_s[b * per + i] = qc[:, i * head_dim : (i + 1) * head_dim].astype(BF16)
    lane_row = lax.broadcasted_iota(jnp.int32, (1, head_dim), 1)
    user_row = jnp.zeros((1, head_dim), F32)
    for i in range(n_cand):
        user_row = jnp.where(lane_row == i, users[i].astype(F32), user_row)
    us_s[0] = user_row

    for b in range(blocks):
        w_copy(0, b).start()
    wo_copy.start()

    def qc_copy(d):
        h = lax.rem(r + d, HEADS)
        return remote(qc_s.at[h], qcz.at[OWN, r], qc_ss.at[d], qc_rs.at[d], in_row(h))

    def us_copy(d):
        h = lax.rem(r + d, HEADS)
        return remote(us_s.at[0], usr.at[OWN, r], us_ss.at[d], us_rs.at[d], in_row(h))

    def qc_arrival(d):
        j = lax.rem(r - d + HEADS, HEADS)
        return remote(qc_s.at[j], qcz.at[OWN, j], qc_ss.at[d], qc_rs.at[d], in_row(j))

    def us_arrival(d):
        j = lax.rem(r - d + HEADS, HEADS)
        return remote(us_s.at[0], usr.at[OWN, j], us_ss.at[d], us_rs.at[d], in_row(j))

    for d in range(1, HEADS):
        qc_copy(d).start()
        us_copy(d).start()
    qcz[OWN, r] = qc_s[r]
    usr[OWN, r] = us_s[0]

    x_copy.wait()

    def norm_body(i, carry):
        part_rows = pl.ds(pl.multiple_of(i * 64, 64), 64)
        nv[part_rows, :] = layer_norm(xv[part_rows, :].astype(F32)).astype(BF16)
        return carry

    lax.fori_loop(0, rows // 64, norm_body, 0)
    bufs = (kbuf, vbuf, qbuf)

    def row_copy(m, h):
        if m == 2:
            return remote(snd.at[m, h], qbuf.at[r], q_ss.at[h], q_rs.at[r], in_row(h))
        return remote(
            snd.at[m, h], bufs[m].at[r], kv_ss.at[m, h], kv_rs.at[m, r], in_row(h)
        )

    def row_arrival(m, j):
        if m == 2:
            return remote(snd.at[m, j], qbuf.at[j], q_ss.at[j], q_rs.at[j], in_row(j))
        return remote(
            snd.at[m, j], bufs[m].at[j], kv_ss.at[m, j], kv_rs.at[m, j], in_row(j)
        )

    def project(mats, first, last):
        def body(i, carry):
            b = block_at(i)
            for m, source in mats:
                if m != 2:
                    w_copy(source, b).wait()
                p = silu(jnp.dot(nv[...], w[source * blocks + b], preferred_element_type=F32))
                if m == 2:
                    p = p * scale
                for i2 in range(per):
                    h = b * per + i2
                    snd[m, h] = p[:, i2 * head_dim : (i2 + 1) * head_dim].astype(BF16)

                    @pl.when(h != r)
                    def _():
                        row_copy(m, h).start()

            return carry

        lax.fori_loop(first, last, body, 0)

    project(((0, 3), (1, 1)), 0, 2)

    def gather_pairs(stage):
        ahead = OWN if stage == 1 else 2 * stage - 3
        behind = OWN if stage == 1 else 5 + 2 * stage
        pairs = [(ahead, 2 * stage - 1, 2), (ahead, 2 * stage - 2, 1)]
        if stage < STAGES:
            pairs.append((behind, 7 + 2 * stage, -2))
        pairs.append((behind, 6 + 2 * stage, -1))
        return pairs

    def gather_copies(stage):
        for src, dst, step in gather_pairs(stage):
            yield remote(qcz.at[src], qcz.at[dst], qg_ss.at[dst], qg_rs.at[dst], along(step))
            yield remote(usr.at[src], usr.at[dst], ug_ss.at[dst], ug_rs.at[dst], along(step))

    for d in range(1, HEADS):
        qc_arrival(d).wait_recv()
        us_arrival(d).wait_recv()
    for copy in gather_copies(1):
        copy.start()

    project(((0, 3), (1, 1)), 2, blocks)
    kbuf[r] = snd[0, r]
    vbuf[r] = snd[1, r]
    project(((2, 2),), 0, blocks)
    qbuf[r] = snd[2, r]

    def qn_copy(h):
        return remote(snd.at[2, h], qnbuf.at[r], qn_ss.at[h], qn_rs.at[r], in_rows(-1, h))

    def qn_arrival(j):
        return remote(snd.at[2, j], qnbuf.at[j], qn_ss.at[j], qn_rs.at[j], in_rows(1, j))

    def qn_sends(first):
        @pl.when(r < PREV)
        def _():
            for i in (first, first + 1):
                qn_copy(lax.rem(r + i + 1, HEADS)).start()

    lane = lax.broadcasted_iota(jnp.int32, (rows, head_dim), 1)
    row_id = lax.broadcasted_iota(jnp.int32, (rows, head_dim), 0)
    total = nz * HEADS * rows

    def owner(j):
        pos = lax.rem((z * HEADS + j) * rows, total) + row_id
        seg = jnp.zeros((rows, head_dim), jnp.int32)
        end = jnp.int32(0)
        for u in range(n_users):
            end = end + lens[u]
            seg = seg + jnp.where(pos >= end, 1, 0)
        return lane == seg

    def ext_body(j, carry):
        mine = owner(j)
        kext[j] = jnp.where(mine, 0.0, -BIG).astype(BF16)
        qext[j] = jnp.where(mine, 1.0, 0.0).astype(BF16)
        qnext[j] = jnp.where(owner(HEADS + j), 1.0, 0.0).astype(BF16)
        return carry

    lax.fori_loop(0, HEADS, ext_body, 0)

    def gather_step(stage):
        for copy in gather_copies(stage - 1):
            copy.wait_recv()
        if stage <= STAGES:
            for copy in gather_copies(stage):
                copy.start()

    n_slot = HEADS * n_cand
    slot_lane = lax.broadcasted_iota(jnp.int32, (n_slot, head_dim), 1)
    slot_row = lax.broadcasted_iota(jnp.int32, (n_slot, head_dim), 0)

    def key_block(j):
        return jnp.concatenate([kbuf[j], kext[j]], axis=1)

    def weigh(h):
        return (h * jnp.tanh(h) + h).astype(BF16)

    def name_users(slots):
        for i in slots:
            named = jnp.concatenate(
                [jnp.broadcast_to(usr[i, j], (n_cand, head_dim)) for j in range(HEADS)], axis=0
            )
            picked = jnp.where(slot_lane == lax.rem(slot_row, n_cand), named, 0.0)
            user = jnp.sum(picked, axis=1, keepdims=True).astype(jnp.int32)
            qce[i] = jnp.where(slot_lane == user, 1.0, 0.0).astype(BF16)

    def chips_shards(*offsets):
        return [lax.rem(2 * (chip + o) + b, HEADS) for o in offsets for b in range(2)]

    near = chips_shards(0, 1, 3)
    far = chips_shards(2)

    def kv_wait(shards):
        for j in shards:

            @pl.when(j != r)
            def _():
                row_arrival(0, j).wait_recv()
                row_arrival(1, j).wait_recv()

    def score(slots, shards, fresh):
        q = jnp.concatenate([qcz[i].reshape(n_slot, head_dim) for i in slots], axis=0)
        ext = jnp.concatenate([qce[i] for i in slots], axis=0)
        qx = jnp.concatenate([q, ext], axis=1)
        if fresh:
            acc = jnp.zeros((len(slots) * n_slot, head_dim), F32)
        else:
            acc = jnp.concatenate([part[i] for i in slots], axis=0)
        for j in shards:
            weight = weigh(contract_last(qx, key_block(j)))
            acc = acc + jnp.dot(weight, vbuf[j], preferred_element_type=F32)
        for a, i in enumerate(slots):
            part[i] = acc[a * n_slot : (a + 1) * n_slot]

    stage_slots = [(2 * k, 2 * k + 1, 8 + 2 * k, 9 + 2 * k) for k in range(STAGES)]
    stage_slots[0] += (OWN,)
    stage_slots[STAGES - 1] = stage_slots[STAGES - 1][:-1]

    def rs_copy(i, step):
        return remote(rs_s.at[i], rs_r.at[i], rs_ss.at[i], rs_rs.at[i], along(step))

    def odd_sends(stage):
        k = STAGES - stage
        rs_s[4 + k] = part[2 * stage - 2].astype(BF16)
        rs_copy(4 + k, -1).start()
        rs_s[12 + k] = part[6 + 2 * stage].astype(BF16)
        rs_copy(12 + k, 1).start()

    gather_step(2)
    qn_sends(0)
    for b in range(blocks):
        w_copy(0, b).wait()
        u = silu(jnp.dot(nv[...], w[b], preferred_element_type=F32))
        uv[:, b * bw : (b + 1) * bw] = u.astype(BF16)
    name_users(stage_slots[0])
    gather_step(3)
    qn_sends(2)
    kv_wait(near)
    score(stage_slots[0], near, True)
    name_users(stage_slots[1])
    score(stage_slots[1], near, True)
    gather_step(4)
    qn_sends(4)
    kv_wait(far)
    score(stage_slots[0], far, False)
    odd_sends(1)
    score(stage_slots[1], far, False)
    odd_sends(2)
    name_users(stage_slots[2])
    score(stage_slots[2], near + far, True)
    odd_sends(3)
    qn_sends(6)
    gather_step(5)
    name_users(stage_slots[3])
    score(stage_slots[3], near + far, True)
    odd_sends(4)

    def arrived(stage):
        k = stage - 1
        low = rs_r[k].astype(F32) + rs_r[4 + k].astype(F32)
        high = rs_r[12 + k].astype(F32)
        if stage > 1:
            high = high + rs_r[8 + k].astype(F32)
        return low, high

    def rs_wait(stage):
        k = stage - 1
        rs_copy(k, -2).wait_recv()
        rs_copy(4 + k, -1).wait_recv()
        if stage > 1:
            rs_copy(8 + k, 2).wait_recv()
        rs_copy(12 + k, 1).wait_recv()

    def rs_step(stage):
        k = stage - 1
        e = 2 * WIN // 2 + 2 - 2 * stage
        if stage == 1:
            rs_s[k] = part[e - 1].astype(BF16)
        else:
            rs_wait(stage - 1)
            low, high = arrived(stage - 1)
            rs_s[k] = (part[e - 1] + low).astype(BF16)
            rs_s[8 + k] = (part[7 + e] + high).astype(BF16)
            rs_copy(8 + k, 2).start()
        rs_copy(k, -2).start()

    one_row = lax.broadcasted_iota(jnp.int32, (rows, rows), 0)
    one_col = lax.broadcasted_iota(jnp.int32, (rows, rows), 1)
    two_row = lax.broadcasted_iota(jnp.int32, (2 * rows, rows), 0)
    two_col = lax.broadcasted_iota(jnp.int32, (2 * rows, rows), 1)

    def at_copy(j):
        return remote(at_s.at[j], at_r.at[r], at_ss.at[j], at_rs.at[r], in_row(j))

    def at_arrival(j):
        return remote(at_s.at[j], at_r.at[j], at_ss.at[j], at_rs.at[j], in_row(j))

    def an_copy(j):
        return remote(an_s.at[j], an_r.at[r], an_ss.at[j], an_rs.at[r], in_rows(1, j))

    def an_arrival(h):
        return remote(an_s.at[0], an_r.at[h], an_ss.at[0], an_rs.at[h], in_rows(-1, h))

    def both(ref, p):
        return ref[2 * p : 2 * p + 2].reshape(2 * rows, head_dim)

    def values(weight, j):
        return jnp.dot(weight, vbuf[j], preferred_element_type=F32)

    def attend_own(p):
        for j in (2 * p, 2 * p + 1):

            @pl.when(j != r)
            def _():
                row_arrival(2, j).wait_recv()

        qx = jnp.concatenate([both(qbuf, p), both(qext, p)], axis=1)
        acc = jnp.zeros((2 * rows, head_dim), F32)
        for j in range(2 * p + 1):
            h = contract_last(qx, key_block(j))
            if j == 2 * p:
                h = jnp.where((two_row >= rows) | (two_col <= two_row), h, -BIG)
            if 2 * p + 1 - j == PREV:
                h = jnp.where((two_row < rows) | (two_col > two_row - rows), h, -BIG)
            acc = acc + values(weigh(h), j)
        h = contract_last(qx[rows:], key_block(2 * p + 1))
        h = jnp.where(one_col <= one_row, h, -BIG)
        at_s[2 * p] = acc[:rows].astype(BF16)
        at_s[2 * p + 1] = (acc[rows:] + values(weigh(h), 2 * p + 1)).astype(BF16)
        for j in (2 * p, 2 * p + 1):

            @pl.when(j != r)
            def _():
                at_copy(j).start()

    def attend_next(p):
        many = 2 * p + 1 < PREV
        qn_arrival(2 * p).wait_recv()
        q = jnp.concatenate([qnbuf[2 * p], qnext[2 * p]], axis=1)
        h = contract_last(q, key_block(2 * p + 1))
        h = jnp.where(one_col > one_row, h, -BIG)
        acc = values(weigh(h), 2 * p + 1)
        if many:
            qn_arrival(2 * p + 1).wait_recv()
            qx = jnp.concatenate([both(qnbuf, p), both(qnext, p)], axis=1)
            more = jnp.zeros((2 * rows, head_dim), F32)
            for j in range(2 * p + 2, HEADS):
                h = contract_last(qx, key_block(j))
                if j == 2 * p + 2:
                    h = jnp.where((two_row < rows) | (two_col > two_row - rows), h, -BIG)
                more = more + values(weigh(h), j)
            acc = acc + more[:rows]
            an_s[2 * p + 1] = more[rows:].astype(BF16)
        an_s[2 * p] = acc.astype(BF16)

    rs_step(1)
    attend_own(0)
    attend_own(1)
    attend_own(2)
    rs_step(2)
    attend_next(0)
    an_copy(0).start()
    an_copy(1).start()
    attend_next(1)
    an_copy(2).start()
    attend_next(2)
    attend_next(3)
    rs_step(3)
    an_copy(3).start()
    an_copy(4).start()
    an_copy(5).start()
    attend_own(3)
    at_r[r] = at_s[r]
    rs_step(4)
    an_copy(6).start()
    u_c = jnp.concatenate(
        [
            silu(jnp.dot(cnormed, w[b], preferred_element_type=F32)).astype(BF16)
            for b in range(blocks)
        ],
        axis=1,
    ).astype(F32)

    rs_wait(4)
    low, high = arrived(4)
    cat_s[...] = (part[OWN] + low + high).reshape(HEADS, n_cand, head_dim)

    def cat_copy(d):
        h = lax.rem(r + d, HEADS)
        return remote(cat_s.at[h], cat_r.at[r], cat_ss.at[d], cat_rs.at[d], in_row(h))

    def cat_arrival(d):
        j = lax.rem(r - d + HEADS, HEADS)
        return remote(cat_s.at[j], cat_r.at[j], cat_ss.at[d], cat_rs.at[d], in_row(j))

    for d in range(1, HEADS):
        cat_copy(d).start()
    cat_r[r] = cat_s[r]

    def at_wait(i, carry):
        at_arrival(lax.rem(r + i + 1, HEADS)).wait_recv()
        return carry

    lax.fori_loop(0, HEADS - 1, at_wait, 0)

    @pl.when(r < PREV)
    def _():
        for h in range(HEADS):
            an_arrival(h).wait_recv()

    @pl.when(r == PREV)
    def _():
        an_r[...] = jnp.zeros_like(an_r)

    def y_body(i, carry):
        part_rows = pl.ds(pl.multiple_of(i * 64, 64), 64)
        a = jnp.concatenate(
            [
                at_r[h, part_rows, :].astype(F32) + an_r[h, part_rows, :].astype(F32)
                for h in range(HEADS)
            ],
            axis=1,
        )
        y = layer_norm(a) * uv[part_rows, :].astype(F32)
        yv[part_rows, :] = y.astype(BF16)
        return carry

    lax.fori_loop(0, rows // 64, y_body, 0)
    wo_copy.wait()
    for b in range(width // 256):
        cols = slice(b * 256, (b + 1) * 256)
        o = jnp.dot(yv[...], wo[:, cols], preferred_element_type=F32)
        x_out[:, cols] = (xv[:, cols].astype(F32) + o).astype(BF16)

    for d in range(1, HEADS):
        cat_arrival(d).wait_recv()
    a = jnp.concatenate([cat_r[h] for h in range(HEADS)], axis=1)
    y_c = (layer_norm(a) * u_c).astype(BF16)
    o = jnp.dot(y_c, wo[...], preferred_element_type=F32)
    c_out[...] = (cand[...].astype(F32) + o).astype(BF16)

    for d in range(1, HEADS):
        qc_copy(d).wait_send()
        us_copy(d).wait_send()
        cat_copy(d).wait_send()
    for stage in range(1, STAGES + 1):
        for copy in gather_copies(stage):
            copy.wait_send()
        k = stage - 1
        rs_copy(k, -2).wait_send()
        rs_copy(4 + k, -1).wait_send()
        if stage > 1:
            rs_copy(8 + k, 2).wait_send()
        rs_copy(12 + k, 1).wait_send()

    def drain(i, carry):
        h = lax.rem(r + i + 1, HEADS)
        for m in range(3):
            row_copy(m, h).wait_send()
        at_copy(h).wait_send()
        an_copy(i).wait_send()
        return carry

    lax.fori_loop(0, HEADS - 1, drain, 0)

    @pl.when(r < PREV)
    def _():
        for h in range(HEADS):
            qn_copy(h).wait_send()


def per_device(nz, history, candidates, lengths, cand_user, w_in, w_out):
    rows, width = history.shape
    n_cand = candidates.shape[0]
    hd = width // HEADS
    bw = 256
    dma = pltpu.SemaphoreType.DMA
    vmem = pl.BlockSpec(memory_space=pltpu.VMEM)
    hbm = pl.BlockSpec(memory_space=pl.ANY)
    scratch = [
        pltpu.SMEM(lengths.shape, jnp.int32),
        pltpu.SMEM(cand_user.shape, jnp.int32),
        pltpu.VMEM(candidates.shape, BF16),
        pltpu.VMEM((4 * width // bw, width, bw), BF16),
        pltpu.VMEM((width, width), BF16),
        pltpu.VMEM((rows, width), BF16),
        pltpu.VMEM((rows, width), BF16),
        pltpu.VMEM((rows, width), BF16),
        pltpu.VMEM((rows, width), BF16),
        pltpu.VMEM((3, HEADS, rows, hd), BF16),
        pltpu.VMEM((HEADS, rows, hd), BF16),
        pltpu.VMEM((HEADS, rows, hd), BF16),
        pltpu.VMEM((HEADS, rows, hd), BF16),
        pltpu.VMEM((HEADS, rows, hd), BF16),
        pltpu.VMEM((HEADS, rows, hd), BF16),
        pltpu.VMEM((HEADS, rows, hd), BF16),
        pltpu.VMEM((HEADS, rows, hd), BF16),
        pltpu.VMEM((HEADS, n_cand, hd), BF16),
        pltpu.VMEM((SLOTS, HEADS, n_cand, hd), BF16),
        pltpu.VMEM((1, 1, hd), F32),
        pltpu.VMEM((SLOTS, HEADS, 1, hd), F32),
        pltpu.VMEM((SLOTS, HEADS * n_cand, hd), BF16),
        pltpu.VMEM((SLOTS, HEADS * n_cand, hd), F32),
        pltpu.VMEM((SLOTS, HEADS * n_cand, hd), BF16),
        pltpu.VMEM((SLOTS, HEADS * n_cand, hd), BF16),
        pltpu.VMEM((HEADS, rows, hd), BF16),
        pltpu.VMEM((HEADS, rows, hd), BF16),
        pltpu.VMEM((HEADS, rows, hd), BF16),
        pltpu.VMEM((HEADS, rows, hd), BF16),
        pltpu.VMEM((HEADS, n_cand, hd), F32),
        pltpu.VMEM((HEADS, n_cand, hd), F32),
        dma((3,)),
        dma((4 * width // bw,)),
        dma,
        dma,
        dma((2, HEADS)),
        dma((2, HEADS)),
        dma((HEADS,)),
        dma((HEADS,)),
        dma((HEADS,)),
        dma((HEADS,)),
        dma((HEADS,)),
        dma((HEADS,)),
        dma((HEADS,)),
        dma((HEADS,)),
        dma((SLOTS,)),
        dma((SLOTS,)),
        dma((SLOTS,)),
        dma((SLOTS,)),
        dma((SLOTS,)),
        dma((SLOTS,)),
        dma((HEADS,)),
        dma((HEADS,)),
        dma((HEADS,)),
        dma((HEADS,)),
        dma((HEADS,)),
        dma((HEADS,)),
    ]
    return pl.pallas_call(
        functools.partial(kernel, nz),
        out_shape=(pltpu.VMEM(history.shape, BF16), pltpu.VMEM(candidates.shape, BF16)),
        in_specs=[hbm] * 6,
        out_specs=(vmem, vmem),
        scratch_shapes=scratch,
        compiler_params=pltpu.CompilerParams(
            collective_id=0, has_side_effects=True, vmem_limit_bytes=60 * 2**20
        ),
    )(lengths, cand_user, candidates, history, w_in, w_out)


def solution(mesh):
    nz = mesh.shape["seq"] // HEADS
    both = ("grp", "seq")
    return jax.shard_map(
        functools.partial(per_device, nz),
        mesh=mesh,
        in_specs=(P(both, None), P(both, None), P("grp"), P(both), P(), P()),
        out_specs=(P(both, None), P(both, None)),
        check_vma=False,
    )
```

```python
import functools

import jax
import jax.numpy as jnp
from jax import lax
from jax.experimental import pallas as pl
from jax.experimental.pallas import tpu as pltpu
from jax.sharding import PartitionSpec as P

HEADS = 8
WIN = 8
PREV = WIN - 1
SLOTS = 16
OWN = SLOTS - 1
EPS = 1e-06
HOPS = {
    0: (15, 1),
    1: (2, -1),
    2: (15, 3),
    3: (2, 1),
    4: (5, -1),
    5: (15, 6),
    6: (5, 1),
    7: (5, 2),
    8: (15, -1),
    9: (10, 1),
    10: (15, -3),
    11: (10, -1),
    12: (13, 1),
    13: (15, -6),
    14: (13, -1),
}
BIG = 2.0**30
MESH = pl.DeviceIdType.MESH
F32 = jnp.float32
BF16 = jnp.bfloat16


def silu(s):
    h = 0.5 * s
    return h * jnp.tanh(h) + h


def layer_norm(rows):
    centred = rows - jnp.mean(rows, axis=-1, keepdims=True)
    return centred * lax.rsqrt(jnp.mean(centred * centred, axis=-1, keepdims=True) + EPS)


def contract_last(a, b):
    return lax.dot_general(a, b, (((1,), (1,)), ((), ())), preferred_element_type=F32)


def kernel(
    nz,
    lens_in,
    users_in,
    cand_in,
    hist,
    w_in,
    w_out,
    x_out,
    c_out,
    lens,
    users,
    cand,
    w,
    wo,
    xv,
    nv,
    uv,
    yv,
    snd,
    kbuf,
    vbuf,
    qbuf,
    qnbuf,
    kext,
    qext,
    qnext,
    qc_s,
    qcz,
    us_s,
    usr,
    qce,
    part,
    rs_s,
    rs_r,
    at_s,
    at_r,
    an_s,
    an_r,
    cat_s,
    cat_r,
    small_sem,
    w_sem,
    wo_sem,
    x_sem,
    kv_ss,
    kv_rs,
    q_ss,
    q_rs,
    qn_ss,
    qn_rs,
    qc_ss,
    qc_rs,
    us_ss,
    us_rs,
    qg_ss,
    qg_rs,
    ug_ss,
    ug_rs,
    rs_ss,
    rs_rs,
    at_ss,
    at_rs,
    an_ss,
    an_rs,
    cat_ss,
    cat_rs,
):
    rows, width = xv.shape
    n_cand = cand.shape[0]
    head_dim = width // HEADS
    n_users = lens.shape[0]
    blocks = w.shape[0] // 4
    bw = w.shape[2]
    me = lax.axis_index("seq")
    z = me // HEADS
    r = lax.rem(me, HEADS)
    chip = r // 2

    def in_row(h):
        return {"seq": z * HEADS + h}

    def in_rows(step, h):
        return {"seq": lax.rem(z + step + nz, nz) * HEADS + h}

    def along(step):
        return in_rows(step, r)

    def remote(src, dst, ss, rs, to):
        return pltpu.make_async_remote_copy(
            src_ref=src, dst_ref=dst, send_sem=ss, recv_sem=rs, device_id=to, device_id_type=MESH
        )

    small = [
        pltpu.make_async_copy(src, dst, small_sem.at[i])
        for i, (src, dst) in enumerate(((cand_in, cand), (users_in, users), (lens_in, lens)))
    ]
    for copy in small:
        copy.start()
    x_copy = pltpu.make_async_copy(hist, xv, x_sem)

    def w_copy(m, b):
        i = m * blocks + b
        return pltpu.make_async_copy(
            w_in.at[0, :, pl.ds(pl.multiple_of(m * width + b * bw, bw), bw)], w.at[i], w_sem.at[i]
        )

    def block_at(i):
        return lax.rem(chip + i + (i // 2) * (1 - 2 * (i % 2)), blocks)

    for b in range(blocks):
        w_copy(2, b).start()
    x_copy.start()
    wo_copy = pltpu.make_async_copy(w_out.at[0], wo, wo_sem)

    barrier = pltpu.get_barrier_semaphore()
    for d in range(1, HEADS):
        pl.semaphore_signal(
            barrier, inc=1, device_id=in_row(lax.rem(r + d, HEADS)), device_id_type=MESH
        )
    for step in (-6, -3, -2, 2, 3, 6):
        pl.semaphore_signal(barrier, inc=1, device_id=along(step), device_id_type=MESH)
    for step in (-1, 1):
        for h in range(HEADS):
            pl.semaphore_signal(barrier, inc=1, device_id=in_rows(step, h), device_id_type=MESH)

    pl.semaphore_wait(barrier, HEADS - 1 + 6 + 2 * HEADS)
    for i in range(blocks):
        w_copy(3, block_at(i)).start()
        w_copy(1, block_at(i)).start()

    scale = 0.5 * head_dim ** (-0.5)
    for copy in small:
        copy.wait()
    cnormed = layer_norm(cand[...].astype(F32)).astype(BF16)
    per = bw // head_dim
    for b in range(blocks):
        w_copy(2, b).wait()
        qc = silu(jnp.dot(cnormed, w[2 * blocks + b], preferred_element_type=F32)) * scale
        for i in range(per):
            qc_s[b * per + i] = qc[:, i * head_dim : (i + 1) * head_dim].astype(BF16)
    lane_row = lax.broadcasted_iota(jnp.int32, (1, head_dim), 1)
    user_row = jnp.zeros((1, head_dim), F32)
    for i in range(n_cand):
        user_row = jnp.where(lane_row == i, users[i].astype(F32), user_row)
    us_s[0] = user_row

    for b in range(blocks):
        w_copy(0, b).start()
    wo_copy.start()

    def qc_copy(d):
        h = lax.rem(r + d, HEADS)
        return remote(qc_s.at[h], qcz.at[OWN, r], qc_ss.at[d], qc_rs.at[d], in_row(h))

    def us_copy(d):
        h = lax.rem(r + d, HEADS)
        return remote(us_s.at[0], usr.at[OWN, r], us_ss.at[d], us_rs.at[d], in_row(h))

    def qc_arrival(d):
        j = lax.rem(r - d + HEADS, HEADS)
        return remote(qc_s.at[j], qcz.at[OWN, j], qc_ss.at[d], qc_rs.at[d], in_row(j))

    def us_arrival(d):
        j = lax.rem(r - d + HEADS, HEADS)
        return remote(us_s.at[0], usr.at[OWN, j], us_ss.at[d], us_rs.at[d], in_row(j))

    for d in range(1, HEADS):
        qc_copy(d).start()
        us_copy(d).start()
    qcz[OWN, r] = qc_s[r]
    usr[OWN, r] = us_s[0]

    x_copy.wait()

    def norm_body(i, carry):
        part_rows = pl.ds(pl.multiple_of(i * 64, 64), 64)
        nv[part_rows, :] = layer_norm(xv[part_rows, :].astype(F32)).astype(BF16)
        return carry

    lax.fori_loop(0, rows // 64, norm_body, 0)
    bufs = (kbuf, vbuf, qbuf)

    def row_copy(m, h):
        if m == 2:
            return remote(snd.at[m, h], qbuf.at[r], q_ss.at[h], q_rs.at[r], in_row(h))
        return remote(
            snd.at[m, h], bufs[m].at[r], kv_ss.at[m, h], kv_rs.at[m, r], in_row(h)
        )

    def row_arrival(m, j):
        if m == 2:
            return remote(snd.at[m, j], qbuf.at[j], q_ss.at[j], q_rs.at[j], in_row(j))
        return remote(
            snd.at[m, j], bufs[m].at[j], kv_ss.at[m, j], kv_rs.at[m, j], in_row(j)
        )

    def project(mats, first, last):
        def body(i, carry):
            b = block_at(i)
            for m, source in mats:
                if m != 2:
                    w_copy(source, b).wait()
                p = silu(jnp.dot(nv[...], w[source * blocks + b], preferred_element_type=F32))
                if m == 2:
                    p = p * scale
                for i2 in range(per):
                    h = b * per + i2
                    snd[m, h] = p[:, i2 * head_dim : (i2 + 1) * head_dim].astype(BF16)

                    @pl.when(h != r)
                    def _():
                        row_copy(m, h).start()

            return carry

        lax.fori_loop(first, last, body, 0)

    project(((0, 3), (1, 1)), 0, 2)

    def gather_copies(slots):
        copies = []
        for dst in slots:
            src, step = HOPS[dst]
            for ref, ss, rs in ((qcz, qg_ss, qg_rs), (usr, ug_ss, ug_rs)):
                copies.append(remote(ref.at[src], ref.at[dst], ss.at[dst], rs.at[dst], along(step)))
        return copies

    def gather_start(*slots):
        for copy in gather_copies(slots):
            copy.start()

    def gather_wait(*slots):
        for copy in gather_copies(slots):
            copy.wait_recv()

    for d in range(1, HEADS):
        qc_arrival(d).wait_recv()
        us_arrival(d).wait_recv()
    gather_start(5, 13, 2, 10, 0, 8)

    project(((0, 3), (1, 1)), 2, blocks)
    kbuf[r] = snd[0, r]
    vbuf[r] = snd[1, r]
    project(((2, 2),), 0, blocks)
    qbuf[r] = snd[2, r]

    def qn_copy(h):
        return remote(snd.at[2, h], qnbuf.at[r], qn_ss.at[h], qn_rs.at[r], in_rows(-1, h))

    def qn_arrival(j):
        return remote(snd.at[2, j], qnbuf.at[j], qn_ss.at[j], qn_rs.at[j], in_rows(1, j))

    def qn_sends(first):
        @pl.when(r < PREV)
        def _():
            for i in (first, first + 1):
                qn_copy(lax.rem(r + i + 1, HEADS)).start()

    qn_sends(0)

    lane = lax.broadcasted_iota(jnp.int32, (rows, head_dim), 1)
    row_id = lax.broadcasted_iota(jnp.int32, (rows, head_dim), 0)
    total = nz * HEADS * rows

    def owner(j):
        pos = lax.rem((z * HEADS + j) * rows, total) + row_id
        seg = jnp.zeros((rows, head_dim), jnp.int32)
        end = jnp.int32(0)
        for u in range(n_users):
            end = end + lens[u]
            seg = seg + jnp.where(pos >= end, 1, 0)
        return lane == seg

    def ext_body(j, carry):
        mine = owner(j)
        kext[j] = jnp.where(mine, 0.0, -BIG).astype(BF16)
        qext[j] = jnp.where(mine, 1.0, 0.0).astype(BF16)
        qnext[j] = jnp.where(owner(HEADS + j), 1.0, 0.0).astype(BF16)
        return carry

    lax.fori_loop(0, HEADS, ext_body, 0)

    n_slot = HEADS * n_cand
    slot_lane = lax.broadcasted_iota(jnp.int32, (n_slot, head_dim), 1)
    slot_row = lax.broadcasted_iota(jnp.int32, (n_slot, head_dim), 0)

    def key_block(j):
        return jnp.concatenate([kbuf[j], kext[j]], axis=1)

    def weigh(h):
        return (h * jnp.tanh(h) + h).astype(BF16)

    def name_users(slots):
        for i in slots:
            named = jnp.concatenate(
                [jnp.broadcast_to(usr[i, j], (n_cand, head_dim)) for j in range(HEADS)], axis=0
            )
            picked = jnp.where(slot_lane == lax.rem(slot_row, n_cand), named, 0.0)
            user = jnp.sum(picked, axis=1, keepdims=True).astype(jnp.int32)
            qce[i] = jnp.where(slot_lane == user, 1.0, 0.0).astype(BF16)

    def chips_shards(*offsets):
        return [lax.rem(2 * (chip + o) + b, HEADS) for o in offsets for b in range(2)]

    near = chips_shards(0, 1, 3)
    far = chips_shards(2)

    def kv_wait(shards):
        for j in shards:

            @pl.when(j != r)
            def _():
                row_arrival(0, j).wait_recv()
                row_arrival(1, j).wait_recv()

    def score(slots, shards, fresh):
        q = jnp.concatenate([qcz[i].reshape(n_slot, head_dim) for i in slots], axis=0)
        ext = jnp.concatenate([qce[i] for i in slots], axis=0)
        qx = jnp.concatenate([q, ext], axis=1)
        if fresh:
            acc = jnp.zeros((len(slots) * n_slot, head_dim), F32)
        else:
            acc = jnp.concatenate([part[i] for i in slots], axis=0)
        for j in shards:
            weight = weigh(contract_last(qx, key_block(j)))
            acc = acc + jnp.dot(weight, vbuf[j], preferred_element_type=F32)
        for a, i in enumerate(slots):
            part[i] = acc[a * n_slot : (a + 1) * n_slot]

    def rs_copy(i):
        return remote(rs_s.at[i], rs_r.at[i], rs_ss.at[i], rs_rs.at[i], along(-HOPS[i][1]))

    def sum_start(*slots):
        for i in slots:
            rs_s[i] = part[i].astype(BF16)
            rs_copy(i).start()

    def arrived(*slots):
        for i in slots:
            rs_copy(i).wait_recv()
        return sum(rs_r[i].astype(F32) for i in slots)

    def relay(i, *slots):
        rs_s[i] = (part[i] + arrived(*slots)).astype(BF16)
        rs_copy(i).start()

    for b in range(blocks):
        w_copy(0, b).wait()
        u = silu(jnp.dot(nv[...], w[b], preferred_element_type=F32))
        uv[:, b * bw : (b + 1) * bw] = u.astype(BF16)
    gather_wait(2, 10)
    gather_start(3, 1, 11, 9)
    qn_sends(2)
    gather_wait(5, 13)
    gather_start(7, 6, 4, 14, 12)
    qn_sends(4)
    gather_wait(0, 8)
    first = (OWN, 0, 8, 2, 10)
    second = (5, 13, 1, 3, 9, 11)
    last = (4, 6, 7, 12, 14)
    name_users(first)
    kv_wait(near)
    score(first, near, True)
    gather_wait(3, 1, 11, 9)
    qn_sends(6)
    name_users(second)
    score(second, near, True)
    gather_wait(7, 6, 4, 14, 12)
    name_users(last)
    kv_wait(far)
    score(last, near + far, True)
    sum_start(*last)
    score(second, far, False)
    sum_start(1, 3, 9, 11)
    score(first, far, False)
    sum_start(0, 8)

    one_row = lax.broadcasted_iota(jnp.int32, (rows, rows), 0)
    one_col = lax.broadcasted_iota(jnp.int32, (rows, rows), 1)
    two_row = lax.broadcasted_iota(jnp.int32, (2 * rows, rows), 0)
    two_col = lax.broadcasted_iota(jnp.int32, (2 * rows, rows), 1)

    def at_copy(j):
        return remote(at_s.at[j], at_r.at[r], at_ss.at[j], at_rs.at[r], in_row(j))

    def at_arrival(j):
        return remote(at_s.at[j], at_r.at[j], at_ss.at[j], at_rs.at[j], in_row(j))

    def an_copy(j):
        return remote(an_s.at[j], an_r.at[r], an_ss.at[j], an_rs.at[r], in_rows(1, j))

    def an_arrival(h):
        return remote(an_s.at[0], an_r.at[h], an_ss.at[0], an_rs.at[h], in_rows(-1, h))

    def both(ref, p):
        return ref[2 * p : 2 * p + 2].reshape(2 * rows, head_dim)

    def values(weight, j):
        return jnp.dot(weight, vbuf[j], preferred_element_type=F32)

    def attend_own(p):
        for j in (2 * p, 2 * p + 1):

            @pl.when(j != r)
            def _():
                row_arrival(2, j).wait_recv()

        qx = jnp.concatenate([both(qbuf, p), both(qext, p)], axis=1)
        acc = jnp.zeros((2 * rows, head_dim), F32)
        for j in range(2 * p + 1):
            h = contract_last(qx, key_block(j))
            if j == 2 * p:
                h = jnp.where((two_row >= rows) | (two_col <= two_row), h, -BIG)
            if 2 * p + 1 - j == PREV:
                h = jnp.where((two_row < rows) | (two_col > two_row - rows), h, -BIG)
            acc = acc + values(weigh(h), j)
        h = contract_last(qx[rows:], key_block(2 * p + 1))
        h = jnp.where(one_col <= one_row, h, -BIG)
        at_s[2 * p] = acc[:rows].astype(BF16)
        at_s[2 * p + 1] = (acc[rows:] + values(weigh(h), 2 * p + 1)).astype(BF16)
        for j in (2 * p, 2 * p + 1):

            @pl.when(j != r)
            def _():
                at_copy(j).start()

    def attend_next(p):
        many = 2 * p + 1 < PREV
        qn_arrival(2 * p).wait_recv()
        q = jnp.concatenate([qnbuf[2 * p], qnext[2 * p]], axis=1)
        h = contract_last(q, key_block(2 * p + 1))
        h = jnp.where(one_col > one_row, h, -BIG)
        acc = values(weigh(h), 2 * p + 1)
        if many:
            qn_arrival(2 * p + 1).wait_recv()
            qx = jnp.concatenate([both(qnbuf, p), both(qnext, p)], axis=1)
            more = jnp.zeros((2 * rows, head_dim), F32)
            for j in range(2 * p + 2, HEADS):
                h = contract_last(qx, key_block(j))
                if j == 2 * p + 2:
                    h = jnp.where((two_row < rows) | (two_col > two_row - rows), h, -BIG)
                more = more + values(weigh(h), j)
            acc = acc + more[:rows]
            an_s[2 * p + 1] = more[rows:].astype(BF16)
        an_s[2 * p] = acc.astype(BF16)

    attend_next(0)
    an_copy(0).start()
    an_copy(1).start()
    attend_next(1)
    relay(5, 4, 6, 7)
    relay(13, 12, 14)
    an_copy(2).start()
    an_copy(3).start()
    relay(2, 1, 3)
    relay(10, 9, 11)
    attend_next(2)
    attend_next(3)
    an_copy(4).start()
    an_copy(5).start()
    an_copy(6).start()
    for p in range(HEADS // 2):
        attend_own(p)
    at_r[r] = at_s[r]
    u_c = jnp.concatenate(
        [
            silu(jnp.dot(cnormed, w[b], preferred_element_type=F32)).astype(BF16)
            for b in range(blocks)
        ],
        axis=1,
    ).astype(F32)

    sums = part[OWN] + arrived(0, 8, 2, 10, 5, 13)
    cat_s[...] = sums.reshape(HEADS, n_cand, head_dim)

    def cat_copy(d):
        h = lax.rem(r + d, HEADS)
        return remote(cat_s.at[h], cat_r.at[r], cat_ss.at[d], cat_rs.at[d], in_row(h))

    def cat_arrival(d):
        j = lax.rem(r - d + HEADS, HEADS)
        return remote(cat_s.at[j], cat_r.at[j], cat_ss.at[d], cat_rs.at[d], in_row(j))

    for d in range(1, HEADS):
        cat_copy(d).start()
    cat_r[r] = cat_s[r]

    def at_wait(i, carry):
        at_arrival(lax.rem(r + i + 1, HEADS)).wait_recv()
        return carry

    lax.fori_loop(0, HEADS - 1, at_wait, 0)

    @pl.when(r < PREV)
    def _():
        for h in range(HEADS):
            an_arrival(h).wait_recv()

    @pl.when(r == PREV)
    def _():
        an_r[...] = jnp.zeros_like(an_r)

    def y_body(i, carry):
        part_rows = pl.ds(pl.multiple_of(i * 64, 64), 64)
        a = jnp.concatenate(
            [
                at_r[h, part_rows, :].astype(F32) + an_r[h, part_rows, :].astype(F32)
                for h in range(HEADS)
            ],
            axis=1,
        )
        y = layer_norm(a) * uv[part_rows, :].astype(F32)
        yv[part_rows, :] = y.astype(BF16)
        return carry

    lax.fori_loop(0, rows // 64, y_body, 0)
    wo_copy.wait()
    for b in range(width // 256):
        cols = slice(b * 256, (b + 1) * 256)
        o = jnp.dot(yv[...], wo[:, cols], preferred_element_type=F32)
        x_out[:, cols] = (xv[:, cols].astype(F32) + o).astype(BF16)

    for d in range(1, HEADS):
        cat_arrival(d).wait_recv()
    a = jnp.concatenate([cat_r[h] for h in range(HEADS)], axis=1)
    y_c = (layer_norm(a) * u_c).astype(BF16)
    o = jnp.dot(y_c, wo[...], preferred_element_type=F32)
    c_out[...] = (cand[...].astype(F32) + o).astype(BF16)

    for d in range(1, HEADS):
        qc_copy(d).wait_send()
        us_copy(d).wait_send()
        cat_copy(d).wait_send()
    for copy in gather_copies(HOPS):
        copy.wait_send()
    for i in HOPS:
        rs_copy(i).wait_send()

    def drain(i, carry):
        h = lax.rem(r + i + 1, HEADS)
        for m in range(3):
            row_copy(m, h).wait_send()
        at_copy(h).wait_send()
        an_copy(i).wait_send()
        return carry

    lax.fori_loop(0, HEADS - 1, drain, 0)

    @pl.when(r < PREV)
    def _():
        for h in range(HEADS):
            qn_copy(h).wait_send()


def per_device(nz, history, candidates, lengths, cand_user, w_in, w_out):
    rows, width = history.shape
    n_cand = candidates.shape[0]
    hd = width // HEADS
    bw = 256
    dma = pltpu.SemaphoreType.DMA
    vmem = pl.BlockSpec(memory_space=pltpu.VMEM)
    hbm = pl.BlockSpec(memory_space=pl.ANY)
    scratch = [
        pltpu.SMEM(lengths.shape, jnp.int32),
        pltpu.SMEM(cand_user.shape, jnp.int32),
        pltpu.VMEM(candidates.shape, BF16),
        pltpu.VMEM((4 * width // bw, width, bw), BF16),
        pltpu.VMEM((width, width), BF16),
        pltpu.VMEM((rows, width), BF16),
        pltpu.VMEM((rows, width), BF16),
        pltpu.VMEM((rows, width), BF16),
        pltpu.VMEM((rows, width), BF16),
        pltpu.VMEM((3, HEADS, rows, hd), BF16),
        pltpu.VMEM((HEADS, rows, hd), BF16),
        pltpu.VMEM((HEADS, rows, hd), BF16),
        pltpu.VMEM((HEADS, rows, hd), BF16),
        pltpu.VMEM((HEADS, rows, hd), BF16),
        pltpu.VMEM((HEADS, rows, hd), BF16),
        pltpu.VMEM((HEADS, rows, hd), BF16),
        pltpu.VMEM((HEADS, rows, hd), BF16),
        pltpu.VMEM((HEADS, n_cand, hd), BF16),
        pltpu.VMEM((SLOTS, HEADS, n_cand, hd), BF16),
        pltpu.VMEM((1, 1, hd), F32),
        pltpu.VMEM((SLOTS, HEADS, 1, hd), F32),
        pltpu.VMEM((SLOTS, HEADS * n_cand, hd), BF16),
        pltpu.VMEM((SLOTS, HEADS * n_cand, hd), F32),
        pltpu.VMEM((SLOTS, HEADS * n_cand, hd), BF16),
        pltpu.VMEM((SLOTS, HEADS * n_cand, hd), BF16),
        pltpu.VMEM((HEADS, rows, hd), BF16),
        pltpu.VMEM((HEADS, rows, hd), BF16),
        pltpu.VMEM((HEADS, rows, hd), BF16),
        pltpu.VMEM((HEADS, rows, hd), BF16),
        pltpu.VMEM((HEADS, n_cand, hd), F32),
        pltpu.VMEM((HEADS, n_cand, hd), F32),
        dma((3,)),
        dma((4 * width // bw,)),
        dma,
        dma,
        dma((2, HEADS)),
        dma((2, HEADS)),
        dma((HEADS,)),
        dma((HEADS,)),
        dma((HEADS,)),
        dma((HEADS,)),
        dma((HEADS,)),
        dma((HEADS,)),
        dma((HEADS,)),
        dma((HEADS,)),
        dma((SLOTS,)),
        dma((SLOTS,)),
        dma((SLOTS,)),
        dma((SLOTS,)),
        dma((SLOTS,)),
        dma((SLOTS,)),
        dma((HEADS,)),
        dma((HEADS,)),
        dma((HEADS,)),
        dma((HEADS,)),
        dma((HEADS,)),
        dma((HEADS,)),
    ]
    return pl.pallas_call(
        functools.partial(kernel, nz),
        out_shape=(pltpu.VMEM(history.shape, BF16), pltpu.VMEM(candidates.shape, BF16)),
        in_specs=[hbm] * 6,
        out_specs=(vmem, vmem),
        scratch_shapes=scratch,
        compiler_params=pltpu.CompilerParams(
            collective_id=0, has_side_effects=True, vmem_limit_bytes=60 * 2**20
        ),
    )(lengths, cand_user, candidates, history, w_in, w_out)


def solution(mesh):
    nz = mesh.shape["seq"] // HEADS
    both = ("grp", "seq")
    return jax.shard_map(
        functools.partial(per_device, nz),
        mesh=mesh,
        in_specs=(P(both, None), P(both, None), P("grp"), P(both), P(), P()),
        out_specs=(P(both, None), P(both, None)),
        check_vma=False,
    )
```

```python
import functools

import jax
import jax.numpy as jnp
from jax import lax
from jax.experimental import pallas as pl
from jax.experimental.pallas import tpu as pltpu
from jax.sharding import PartitionSpec as P

HEADS = 8
WIN = 8
PREV = WIN - 1
SLOTS = 16
OWN = SLOTS - 1
EPS = 1e-06
HOPS = {
    0: (15, 1),
    1: (2, -1),
    2: (15, 3),
    3: (2, 1),
    4: (5, -1),
    5: (15, 6),
    6: (5, 1),
    7: (5, 2),
    8: (15, -1),
    9: (10, 1),
    10: (15, -3),
    11: (10, -1),
    12: (13, 1),
    13: (15, -6),
    14: (13, -1),
}
BIG = 2.0**30
MESH = pl.DeviceIdType.MESH
F32 = jnp.float32
BF16 = jnp.bfloat16


def silu(s):
    h = 0.5 * s
    return h * jnp.tanh(h) + h


def layer_norm(rows):
    centred = rows - jnp.mean(rows, axis=-1, keepdims=True)
    return centred * lax.rsqrt(jnp.mean(centred * centred, axis=-1, keepdims=True) + EPS)


def contract_last(a, b):
    return lax.dot_general(a, b, (((1,), (1,)), ((), ())), preferred_element_type=F32)


def kernel(
    nz,
    lens_in,
    users_in,
    cand_in,
    hist,
    w_in,
    w_out,
    x_out,
    c_out,
    lens,
    users,
    cand,
    w,
    wo,
    xv,
    nv,
    uv,
    yv,
    snd,
    kbuf,
    vbuf,
    qbuf,
    qnbuf,
    kext,
    qext,
    qnext,
    qc_s,
    qcz,
    us_s,
    usr,
    qce,
    part,
    rs_s,
    rs_r,
    at_s,
    at_r,
    an_s,
    an_r,
    cat_s,
    cat_r,
    small_sem,
    w_sem,
    wo_sem,
    x_sem,
    kv_ss,
    kv_rs,
    q_ss,
    q_rs,
    qn_ss,
    qn_rs,
    qc_ss,
    qc_rs,
    us_ss,
    us_rs,
    qg_ss,
    qg_rs,
    ug_ss,
    ug_rs,
    rs_ss,
    rs_rs,
    at_ss,
    at_rs,
    an_ss,
    an_rs,
    cat_ss,
    cat_rs,
):
    rows, width = xv.shape
    n_cand = cand.shape[0]
    head_dim = width // HEADS
    n_users = lens.shape[0]
    blocks = w.shape[0] // 4
    bw = w.shape[2]
    me = lax.axis_index("seq")
    z = me // HEADS
    r = lax.rem(me, HEADS)
    chip = r // 2

    def in_row(h):
        return {"seq": z * HEADS + h}

    def in_rows(step, h):
        return {"seq": lax.rem(z + step + nz, nz) * HEADS + h}

    def along(step):
        return in_rows(step, r)

    def remote(src, dst, ss, rs, to):
        return pltpu.make_async_remote_copy(
            src_ref=src, dst_ref=dst, send_sem=ss, recv_sem=rs, device_id=to, device_id_type=MESH
        )

    small = [
        pltpu.make_async_copy(src, dst, small_sem.at[i])
        for i, (src, dst) in enumerate(((cand_in, cand), (users_in, users), (lens_in, lens)))
    ]
    for copy in small:
        copy.start()
    x_copy = pltpu.make_async_copy(hist, xv, x_sem)

    def w_copy(m, b):
        i = m * blocks + b
        return pltpu.make_async_copy(
            w_in.at[0, :, pl.ds(pl.multiple_of(m * width + b * bw, bw), bw)], w.at[i], w_sem.at[i]
        )

    def block_at(i):
        return lax.rem(chip + i + (i // 2) * (1 - 2 * (i % 2)), blocks)

    for b in range(blocks):
        w_copy(2, b).start()
    x_copy.start()
    wo_copy = pltpu.make_async_copy(w_out.at[0], wo, wo_sem)

    barrier = pltpu.get_barrier_semaphore()
    for d in range(1, HEADS):
        pl.semaphore_signal(
            barrier, inc=1, device_id=in_row(lax.rem(r + d, HEADS)), device_id_type=MESH
        )
    for step in (-6, -3, -2, 2, 3, 6):
        pl.semaphore_signal(barrier, inc=1, device_id=along(step), device_id_type=MESH)
    for step in (-1, 1):
        for h in range(HEADS):
            pl.semaphore_signal(barrier, inc=1, device_id=in_rows(step, h), device_id_type=MESH)

    scale = 0.5 * head_dim ** (-0.5)
    for copy in small:
        copy.wait()
    cnormed = layer_norm(cand[...].astype(F32)).astype(BF16)
    per = bw // head_dim
    for b in range(blocks):
        w_copy(2, b).wait()
        if b == 0:
            for i in range(blocks):
                w_copy(3, block_at(i)).start()
                w_copy(1, block_at(i)).start()
        qc = silu(jnp.dot(cnormed, w[2 * blocks + b], preferred_element_type=F32)) * scale
        for i in range(per):
            qc_s[b * per + i] = qc[:, i * head_dim : (i + 1) * head_dim].astype(BF16)
    lane_row = lax.broadcasted_iota(jnp.int32, (1, head_dim), 1)
    user_row = jnp.zeros((1, head_dim), F32)
    for i in range(n_cand):
        user_row = jnp.where(lane_row == i, users[i].astype(F32), user_row)
    us_s[0] = user_row

    for b in range(blocks):
        w_copy(0, b).start()
    wo_copy.start()

    def qc_copy(d):
        h = lax.rem(r + d, HEADS)
        return remote(qc_s.at[h], qcz.at[OWN, r], qc_ss.at[d], qc_rs.at[d], in_row(h))

    def us_copy(d):
        h = lax.rem(r + d, HEADS)
        return remote(us_s.at[0], usr.at[OWN, r], us_ss.at[d], us_rs.at[d], in_row(h))

    def qc_arrival(d):
        j = lax.rem(r - d + HEADS, HEADS)
        return remote(qc_s.at[j], qcz.at[OWN, j], qc_ss.at[d], qc_rs.at[d], in_row(j))

    def us_arrival(d):
        j = lax.rem(r - d + HEADS, HEADS)
        return remote(us_s.at[0], usr.at[OWN, j], us_ss.at[d], us_rs.at[d], in_row(j))

    pl.semaphore_wait(barrier, HEADS - 1 + 6 + 2 * HEADS)
    for d in range(1, HEADS):
        qc_copy(d).start()
        us_copy(d).start()
    qcz[OWN, r] = qc_s[r]
    usr[OWN, r] = us_s[0]

    x_copy.wait()

    def norm_body(i, carry):
        part_rows = pl.ds(pl.multiple_of(i * 64, 64), 64)
        nv[part_rows, :] = layer_norm(xv[part_rows, :].astype(F32)).astype(BF16)
        return carry

    lax.fori_loop(0, rows // 64, norm_body, 0)
    bufs = (kbuf, vbuf, qbuf)

    def row_copy(m, h):
        if m == 2:
            return remote(snd.at[m, h], qbuf.at[r], q_ss.at[h], q_rs.at[r], in_row(h))
        return remote(
            snd.at[m, h], bufs[m].at[r], kv_ss.at[m, h], kv_rs.at[m, r], in_row(h)
        )

    def row_arrival(m, j):
        if m == 2:
            return remote(snd.at[m, j], qbuf.at[j], q_ss.at[j], q_rs.at[j], in_row(j))
        return remote(
            snd.at[m, j], bufs[m].at[j], kv_ss.at[m, j], kv_rs.at[m, j], in_row(j)
        )

    def project(mats, first, last):
        def body(i, carry):
            b = block_at(i)
            for m, source in mats:
                if m != 2:
                    w_copy(source, b).wait()
                p = silu(jnp.dot(nv[...], w[source * blocks + b], preferred_element_type=F32))
                if m == 2:
                    p = p * scale
                for i2 in range(per):
                    h = b * per + i2
                    snd[m, h] = p[:, i2 * head_dim : (i2 + 1) * head_dim].astype(BF16)

                    @pl.when(h != r)
                    def _():
                        row_copy(m, h).start()

            return carry

        lax.fori_loop(first, last, body, 0)

    project(((0, 3), (1, 1)), 0, 2)

    def gather_copies(slots):
        copies = []
        for dst in slots:
            src, step = HOPS[dst]
            for ref, ss, rs in ((qcz, qg_ss, qg_rs), (usr, ug_ss, ug_rs)):
                copies.append(remote(ref.at[src], ref.at[dst], ss.at[dst], rs.at[dst], along(step)))
        return copies

    def gather_start(*slots):
        for copy in gather_copies(slots):
            copy.start()

    def gather_wait(*slots):
        for copy in gather_copies(slots):
            copy.wait_recv()

    for d in range(1, HEADS):
        qc_arrival(d).wait_recv()
        us_arrival(d).wait_recv()
    gather_start(5, 13, 2, 10, 0, 8)

    project(((0, 3), (1, 1)), 2, blocks)
    kbuf[r] = snd[0, r]
    vbuf[r] = snd[1, r]
    project(((2, 2),), 0, blocks)
    qbuf[r] = snd[2, r]

    def qn_copy(h):
        return remote(snd.at[2, h], qnbuf.at[r], qn_ss.at[h], qn_rs.at[r], in_rows(-1, h))

    def qn_arrival(j):
        return remote(snd.at[2, j], qnbuf.at[j], qn_ss.at[j], qn_rs.at[j], in_rows(1, j))

    def qn_sends(first):
        @pl.when(r < PREV)
        def _():
            for i in (first, first + 1):
                qn_copy(lax.rem(r + i + 1, HEADS)).start()

    qn_sends(0)

    lane = lax.broadcasted_iota(jnp.int32, (rows, head_dim), 1)
    row_id = lax.broadcasted_iota(jnp.int32, (rows, head_dim), 0)
    total = nz * HEADS * rows

    def owner(j):
        pos = lax.rem((z * HEADS + j) * rows, total) + row_id
        seg = jnp.zeros((rows, head_dim), jnp.int32)
        end = jnp.int32(0)
        for u in range(n_users):
            end = end + lens[u]
            seg = seg + jnp.where(pos >= end, 1, 0)
        return lane == seg

    def ext_body(j, carry):
        mine = owner(j)
        kext[j] = jnp.where(mine, 0.0, -BIG).astype(BF16)
        qext[j] = jnp.where(mine, 1.0, 0.0).astype(BF16)
        qnext[j] = jnp.where(owner(HEADS + j), 1.0, 0.0).astype(BF16)
        return carry

    lax.fori_loop(0, HEADS, ext_body, 0)

    n_slot = HEADS * n_cand
    slot_lane = lax.broadcasted_iota(jnp.int32, (n_slot, head_dim), 1)
    slot_row = lax.broadcasted_iota(jnp.int32, (n_slot, head_dim), 0)

    def key_block(j):
        return jnp.concatenate([kbuf[j], kext[j]], axis=1)

    def weigh(h):
        return (h * jnp.tanh(h) + h).astype(BF16)

    def name_users(slots):
        for i in slots:
            named = jnp.concatenate(
                [jnp.broadcast_to(usr[i, j], (n_cand, head_dim)) for j in range(HEADS)], axis=0
            )
            picked = jnp.where(slot_lane == lax.rem(slot_row, n_cand), named, 0.0)
            user = jnp.sum(picked, axis=1, keepdims=True).astype(jnp.int32)
            qce[i] = jnp.where(slot_lane == user, 1.0, 0.0).astype(BF16)

    def chips_shards(*offsets):
        return [lax.rem(2 * (chip + o) + b, HEADS) for o in offsets for b in range(2)]

    near = chips_shards(0, 1, 3)
    far = chips_shards(2)

    def kv_wait(shards):
        for j in shards:

            @pl.when(j != r)
            def _():
                row_arrival(0, j).wait_recv()
                row_arrival(1, j).wait_recv()

    def score(slots, shards, fresh):
        q = jnp.concatenate([qcz[i].reshape(n_slot, head_dim) for i in slots], axis=0)
        ext = jnp.concatenate([qce[i] for i in slots], axis=0)
        qx = jnp.concatenate([q, ext], axis=1)
        if fresh:
            acc = jnp.zeros((len(slots) * n_slot, head_dim), F32)
        else:
            acc = jnp.concatenate([part[i] for i in slots], axis=0)
        for j in shards:
            weight = weigh(contract_last(qx, key_block(j)))
            acc = acc + jnp.dot(weight, vbuf[j], preferred_element_type=F32)
        for a, i in enumerate(slots):
            part[i] = acc[a * n_slot : (a + 1) * n_slot]

    def rs_copy(i):
        return remote(rs_s.at[i], rs_r.at[i], rs_ss.at[i], rs_rs.at[i], along(-HOPS[i][1]))

    def sum_start(*slots):
        for i in slots:
            rs_s[i] = part[i].astype(BF16)
            rs_copy(i).start()

    def arrived(*slots):
        for i in slots:
            rs_copy(i).wait_recv()
        return sum(rs_r[i].astype(F32) for i in slots)

    def relay(i, *slots):
        rs_s[i] = (part[i] + arrived(*slots)).astype(BF16)
        rs_copy(i).start()

    for b in range(blocks):
        w_copy(0, b).wait()
        u = silu(jnp.dot(nv[...], w[b], preferred_element_type=F32))
        uv[:, b * bw : (b + 1) * bw] = u.astype(BF16)
    gather_wait(2, 10)
    gather_start(3, 1, 11, 9)
    qn_sends(2)
    gather_wait(5, 13)
    gather_start(7, 6, 4, 14, 12)
    qn_sends(4)
    gather_wait(0, 8)
    first = (OWN, 0, 8, 2, 10)
    second = (5, 13, 1, 3, 9, 11)
    last = (4, 6, 7, 12, 14)
    name_users(first)
    kv_wait(near)
    score(first, near, True)
    gather_wait(3, 1, 11, 9)
    qn_sends(6)
    name_users(second)
    score(second, near, True)
    gather_wait(7, 6, 4, 14, 12)
    name_users(last)
    kv_wait(far)
    score(last, near + far, True)
    sum_start(*last)
    score(second, far, False)
    sum_start(1, 3, 9, 11)
    score(first, far, False)
    sum_start(0, 8)

    one_row = lax.broadcasted_iota(jnp.int32, (rows, rows), 0)
    one_col = lax.broadcasted_iota(jnp.int32, (rows, rows), 1)
    two_row = lax.broadcasted_iota(jnp.int32, (2 * rows, rows), 0)
    two_col = lax.broadcasted_iota(jnp.int32, (2 * rows, rows), 1)

    def at_copy(j):
        return remote(at_s.at[j], at_r.at[r], at_ss.at[j], at_rs.at[r], in_row(j))

    def at_arrival(j):
        return remote(at_s.at[j], at_r.at[j], at_ss.at[j], at_rs.at[j], in_row(j))

    def an_copy(j):
        return remote(an_s.at[j], an_r.at[r], an_ss.at[j], an_rs.at[r], in_rows(1, j))

    def an_arrival(h):
        return remote(an_s.at[0], an_r.at[h], an_ss.at[0], an_rs.at[h], in_rows(-1, h))

    def both(ref, p):
        return ref[2 * p : 2 * p + 2].reshape(2 * rows, head_dim)

    def values(weight, j):
        return jnp.dot(weight, vbuf[j], preferred_element_type=F32)

    def attend_own(p):
        for j in (2 * p, 2 * p + 1):

            @pl.when(j != r)
            def _():
                row_arrival(2, j).wait_recv()

        qx = jnp.concatenate([both(qbuf, p), both(qext, p)], axis=1)
        acc = jnp.zeros((2 * rows, head_dim), F32)
        for j in range(2 * p + 1):
            h = contract_last(qx, key_block(j))
            if j == 2 * p:
                h = jnp.where((two_row >= rows) | (two_col <= two_row), h, -BIG)
            if 2 * p + 1 - j == PREV:
                h = jnp.where((two_row < rows) | (two_col > two_row - rows), h, -BIG)
            acc = acc + values(weigh(h), j)
        h = contract_last(qx[rows:], key_block(2 * p + 1))
        h = jnp.where(one_col <= one_row, h, -BIG)
        at_s[2 * p] = acc[:rows].astype(BF16)
        at_s[2 * p + 1] = (acc[rows:] + values(weigh(h), 2 * p + 1)).astype(BF16)
        for j in (2 * p, 2 * p + 1):

            @pl.when(j != r)
            def _():
                at_copy(j).start()

    def attend_next(p):
        many = 2 * p + 1 < PREV
        qn_arrival(2 * p).wait_recv()
        q = jnp.concatenate([qnbuf[2 * p], qnext[2 * p]], axis=1)
        h = contract_last(q, key_block(2 * p + 1))
        h = jnp.where(one_col > one_row, h, -BIG)
        acc = values(weigh(h), 2 * p + 1)
        if many:
            qn_arrival(2 * p + 1).wait_recv()
            qx = jnp.concatenate([both(qnbuf, p), both(qnext, p)], axis=1)
            more = jnp.zeros((2 * rows, head_dim), F32)
            for j in range(2 * p + 2, HEADS):
                h = contract_last(qx, key_block(j))
                if j == 2 * p + 2:
                    h = jnp.where((two_row < rows) | (two_col > two_row - rows), h, -BIG)
                more = more + values(weigh(h), j)
            acc = acc + more[:rows]
            an_s[2 * p + 1] = more[rows:].astype(BF16)
        an_s[2 * p] = acc.astype(BF16)

    attend_next(0)
    an_copy(0).start()
    an_copy(1).start()
    attend_next(1)
    relay(5, 4, 6, 7)
    relay(13, 12, 14)
    an_copy(2).start()
    an_copy(3).start()
    relay(2, 1, 3)
    relay(10, 9, 11)
    attend_next(2)
    attend_next(3)
    an_copy(4).start()
    an_copy(5).start()
    an_copy(6).start()
    for p in range(HEADS // 2):
        attend_own(p)
    at_r[r] = at_s[r]
    u_c = jnp.concatenate(
        [
            silu(jnp.dot(cnormed, w[b], preferred_element_type=F32)).astype(BF16)
            for b in range(blocks)
        ],
        axis=1,
    ).astype(F32)

    sums = part[OWN] + arrived(0, 8, 2, 10, 5, 13)
    cat_s[...] = sums.reshape(HEADS, n_cand, head_dim)

    def cat_copy(d):
        h = lax.rem(r + d, HEADS)
        return remote(cat_s.at[h], cat_r.at[r], cat_ss.at[d], cat_rs.at[d], in_row(h))

    def cat_arrival(d):
        j = lax.rem(r - d + HEADS, HEADS)
        return remote(cat_s.at[j], cat_r.at[j], cat_ss.at[d], cat_rs.at[d], in_row(j))

    for d in range(1, HEADS):
        cat_copy(d).start()
    cat_r[r] = cat_s[r]

    def at_wait(i, carry):
        at_arrival(lax.rem(r + i + 1, HEADS)).wait_recv()
        return carry

    lax.fori_loop(0, HEADS - 1, at_wait, 0)

    @pl.when(r < PREV)
    def _():
        for h in range(HEADS):
            an_arrival(h).wait_recv()

    @pl.when(r == PREV)
    def _():
        an_r[...] = jnp.zeros_like(an_r)

    def y_body(i, carry):
        part_rows = pl.ds(pl.multiple_of(i * 64, 64), 64)
        a = jnp.concatenate(
            [
                at_r[h, part_rows, :].astype(F32) + an_r[h, part_rows, :].astype(F32)
                for h in range(HEADS)
            ],
            axis=1,
        )
        y = layer_norm(a) * uv[part_rows, :].astype(F32)
        yv[part_rows, :] = y.astype(BF16)
        return carry

    lax.fori_loop(0, rows // 64, y_body, 0)
    wo_copy.wait()
    for b in range(width // 256):
        cols = slice(b * 256, (b + 1) * 256)
        o = jnp.dot(yv[...], wo[:, cols], preferred_element_type=F32)
        x_out[:, cols] = (xv[:, cols].astype(F32) + o).astype(BF16)

    for d in range(1, HEADS):
        cat_arrival(d).wait_recv()
    a = jnp.concatenate([cat_r[h] for h in range(HEADS)], axis=1)
    y_c = (layer_norm(a) * u_c).astype(BF16)
    o = jnp.dot(y_c, wo[...], preferred_element_type=F32)
    c_out[...] = (cand[...].astype(F32) + o).astype(BF16)

    for d in range(1, HEADS):
        qc_copy(d).wait_send()
        us_copy(d).wait_send()
        cat_copy(d).wait_send()
    for copy in gather_copies(HOPS):
        copy.wait_send()
    for i in HOPS:
        rs_copy(i).wait_send()

    def drain(i, carry):
        h = lax.rem(r + i + 1, HEADS)
        for m in range(3):
            row_copy(m, h).wait_send()
        at_copy(h).wait_send()
        an_copy(i).wait_send()
        return carry

    lax.fori_loop(0, HEADS - 1, drain, 0)

    @pl.when(r < PREV)
    def _():
        for h in range(HEADS):
            qn_copy(h).wait_send()


def per_device(nz, history, candidates, lengths, cand_user, w_in, w_out):
    rows, width = history.shape
    n_cand = candidates.shape[0]
    hd = width // HEADS
    bw = 256
    dma = pltpu.SemaphoreType.DMA
    vmem = pl.BlockSpec(memory_space=pltpu.VMEM)
    hbm = pl.BlockSpec(memory_space=pl.ANY)
    scratch = [
        pltpu.SMEM(lengths.shape, jnp.int32),
        pltpu.SMEM(cand_user.shape, jnp.int32),
        pltpu.VMEM(candidates.shape, BF16),
        pltpu.VMEM((4 * width // bw, width, bw), BF16),
        pltpu.VMEM((width, width), BF16),
        pltpu.VMEM((rows, width), BF16),
        pltpu.VMEM((rows, width), BF16),
        pltpu.VMEM((rows, width), BF16),
        pltpu.VMEM((rows, width), BF16),
        pltpu.VMEM((3, HEADS, rows, hd), BF16),
        pltpu.VMEM((HEADS, rows, hd), BF16),
        pltpu.VMEM((HEADS, rows, hd), BF16),
        pltpu.VMEM((HEADS, rows, hd), BF16),
        pltpu.VMEM((HEADS, rows, hd), BF16),
        pltpu.VMEM((HEADS, rows, hd), BF16),
        pltpu.VMEM((HEADS, rows, hd), BF16),
        pltpu.VMEM((HEADS, rows, hd), BF16),
        pltpu.VMEM((HEADS, n_cand, hd), BF16),
        pltpu.VMEM((SLOTS, HEADS, n_cand, hd), BF16),
        pltpu.VMEM((1, 1, hd), F32),
        pltpu.VMEM((SLOTS, HEADS, 1, hd), F32),
        pltpu.VMEM((SLOTS, HEADS * n_cand, hd), BF16),
        pltpu.VMEM((SLOTS, HEADS * n_cand, hd), F32),
        pltpu.VMEM((SLOTS, HEADS * n_cand, hd), BF16),
        pltpu.VMEM((SLOTS, HEADS * n_cand, hd), BF16),
        pltpu.VMEM((HEADS, rows, hd), BF16),
        pltpu.VMEM((HEADS, rows, hd), BF16),
        pltpu.VMEM((HEADS, rows, hd), BF16),
        pltpu.VMEM((HEADS, rows, hd), BF16),
        pltpu.VMEM((HEADS, n_cand, hd), F32),
        pltpu.VMEM((HEADS, n_cand, hd), F32),
        dma((3,)),
        dma((4 * width // bw,)),
        dma,
        dma,
        dma((2, HEADS)),
        dma((2, HEADS)),
        dma((HEADS,)),
        dma((HEADS,)),
        dma((HEADS,)),
        dma((HEADS,)),
        dma((HEADS,)),
        dma((HEADS,)),
        dma((HEADS,)),
        dma((HEADS,)),
        dma((SLOTS,)),
        dma((SLOTS,)),
        dma((SLOTS,)),
        dma((SLOTS,)),
        dma((SLOTS,)),
        dma((SLOTS,)),
        dma((HEADS,)),
        dma((HEADS,)),
        dma((HEADS,)),
        dma((HEADS,)),
        dma((HEADS,)),
        dma((HEADS,)),
    ]
    return pl.pallas_call(
        functools.partial(kernel, nz),
        out_shape=(pltpu.VMEM(history.shape, BF16), pltpu.VMEM(candidates.shape, BF16)),
        in_specs=[hbm] * 6,
        out_specs=(vmem, vmem),
        scratch_shapes=scratch,
        compiler_params=pltpu.CompilerParams(
            collective_id=0, has_side_effects=True, vmem_limit_bytes=60 * 2**20
        ),
    )(lengths, cand_user, candidates, history, w_in, w_out)


def solution(mesh):
    nz = mesh.shape["seq"] // HEADS
    both = ("grp", "seq")
    return jax.shard_map(
        functools.partial(per_device, nz),
        mesh=mesh,
        in_specs=(P(both, None), P(both, None), P("grp"), P(both), P(), P()),
        out_specs=(P(both, None), P(both, None)),
        check_vma=False,
    )
```
